256 devices in a mesh: copy: 32 (over y, z_lo, core), tok: 8 (over z_hi, x).
Axes of the slice: x: 4, y: 4, z: 8 (z_hi: 2, z_lo: 4; z = z_hi * 4 + z_lo), core: 2. Of those that a mesh axis runs over, the one named last changes fastest.
Arguments:
- noisy: bfloat16 [32, 1024, 768], P('copy', 'tok'), may hold values from -6 to 6
- single: bfloat16 [1024, 768], P('tok'), may hold values from -6 to 6
- pair: bfloat16 [1024, 1024, 128], P('tok', 'copy'), may hold values from -6 to 6
- restype: int32 [1024], P('tok'), may hold values from 0 to 31
- chain: int32 [1024], replicated, may hold values from 0 to 5, never falling along the last dimension, each value on 1 to 512 neighbouring positions
- keymask: int32 [1024], replicated, may hold values from 0 to 1, as said below
- restype_table: bfloat16 [32, 768], replicated, may hold values from -3 to 3
- norm_gain: float32 [768], replicated, may hold values from 0.25 to 1.75
- pair_gain: float32 [128], replicated, may hold values from 0.25 to 1.75
- trans_gain: float32 [768], replicated, may hold values from 0.25 to 1.75
- w_query: bfloat16 [768, 768], replicated, may hold values from -0.21875 to 0.21875
- w_key: bfloat16 [768, 768], replicated, may hold values from -0.21875 to 0.21875
- w_value: bfloat16 [768, 768], replicated, may hold values from -0.21875 to 0.21875
- w_out: bfloat16 [768, 768], replicated, may hold values from -0.21875 to 0.21875
- w_pair: bfloat16 [128, 8], replicated, may hold values from -0.5 to 0.5
- chain_weight: float32 [6, 8], replicated, may hold values from -80 to 240
- w_hidden_gate: bfloat16 [768, 1536], replicated, may hold values from -0.21875 to 0.21875
- w_hidden_up: bfloat16 [768, 1536], replicated, may hold values from -0.21875 to 0.21875
- w_down: bfloat16 [1536, 768], replicated, may hold values from -0.15625 to 0.15625
- cotangent: bfloat16 [32, 1024, 768], P('copy', 'tok'), may hold values from -6 to 6
Outputs:
- grad_noisy: bfloat16 [32, 1024, 768], P('copy', 'tok')
- grad_single: float32 [1024, 768], P('tok', 'copy')
- grad_pair: bfloat16 [1024, 1024, 128], P('tok', 'copy')
- grad_query: float32 [768, 768], P('tok', 'copy')
- grad_key: float32 [768, 768], P('tok', 'copy')
- grad_value: float32 [768, 768], P('tok', 'copy')
- grad_out: float32 [768, 768], P('tok', 'copy')
- grad_pair_weight: float32 [128, 8], replicated
The draws below stay inside these ranges and needn't reach their ends.
Inputs may be any that keep to these rules, and one draw needn't show every extreme that they name: `keymask`: 1 on the first positions of the crop and 0 after them, with at least 512 ones. chain numbers never fall along the crop.
All inputs are finite; a program needn't handle non-finite values.
Results may differ from the reference program's by a relative error of at most 0.03.
Values may be sent and summed in bfloat16 or wider, within the bound.
A program may use at most 128 MiB of HBM per device.

```python
import math
import jax
import jax.numpy as jnp
import numpy as np
from jax import lax

D = 768
H = 8
HD = 96
CZ = 128
FF = 1536
RES_TYPES = 32
CHAINS = 6
N = 1024
COPIES = 32


def draw_keymask(key, part):
    length = jax.random.randint(key, (), N // 2, N + 1)
    return (jnp.arange(N, dtype=jnp.int32) < length).astype(jnp.int32)


def draw_chain_weight(key, part):
    return jax.random.uniform(key, (CHAINS, H), jnp.float32, -2.0, 2.0)


def place_ends(drawn, stream_key, smallest, high):
    index_at = [jax.random.randint(jax.random.fold_in(stream_key, axis), (), 0, length) for axis, length in enumerate(drawn.shape)]
    widest = drawn.shape.index(max(drawn.shape))
    neighbour = index_at[:widest] + [(index_at[widest] + 1) % drawn.shape[widest]] + index_at[widest + 1:]
    return drawn.at[tuple(index_at)].set(smallest).at[tuple(neighbour)].set(high)


def block_levels(key, extent, split, low, largest):
    level, own = 1.0, jax.random.fold_in(key, 6)
    for dim, blocks in split:
        heights = jnp.exp(jax.random.uniform(jax.random.fold_in(own, dim), (blocks,), jnp.float32, low / len(split), largest / len(split)))
        level = level * jnp.repeat(heights, extent[dim] // blocks).reshape([-1 if axis == dim else 1 for axis in range(len(extent))])
    return level


def split_up(number_of, total, reach, skew):
    loads = [(1 << 20) // math.isqrt(rank ** skew) + 1 for rank in range(2, number_of + 1)]
    rest, given = total - reach - (number_of - 1), [1] * (number_of - 1)
    while rest > 0:
        candidates = [i for i in range(number_of - 1) if given[i] < reach]
        mass, budget = sum([loads[i] for i in candidates]), rest
        for i in candidates:
            more = min(reach - given[i], max(1, budget * loads[i] // mass), rest)
            given[i] = given[i] + more
            rest = rest - more
    return np.array([reach] + given)


def uneven(key, number_of, total, most, lean):
    if number_of == 2:
        one = jax.random.randint(key, (), max(1, total - most), min(most, total - 1) + 1)
        return jnp.stack([one, total - one])
    tallies = jnp.asarray(split_up(number_of, total, most, lean), jnp.int32)
    twos = (number_of - 1) // 2
    source_of, taker = tallies[1:1 + 2 * twos:2], tallies[2:2 + 2 * twos:2]
    room = jnp.minimum(source_of - 1, most - taker)
    moved = jax.random.randint(jax.random.fold_in(key, 1), (twos,), 0, 1 << 20) % (room + 1)
    tallies = tallies.at[1:1 + 2 * twos:2].set(source_of - moved).at[2:2 + 2 * twos:2].set(taker + moved)
    return tallies[jax.random.permutation(jax.random.fold_in(key, 2), number_of)]


def scatter_about(key, extent, spread, reach, split=(), kind=jnp.bfloat16):
    level = block_levels(key, extent, split, -0.22, 0.18) if split else 1.0
    drawn = jax.random.normal(key, extent, jnp.float32) * spread * level
    return jnp.minimum(jnp.maximum(drawn, -reach), reach).astype(kind)


def setup_inputs(seed: int = 0) -> dict:
    key_list = jax.random.split(jax.random.key(seed), 21)
    return {
        "noisy": scatter_about(key_list[0], (COPIES, N, D), 1.0, 6.0, ((0, 32), (1, 8))),
        "single": scatter_about(key_list[1], (N, D), 1.0, 6.0, ((0, 8),)),
        "pair": scatter_about(key_list[2], (N, N, CZ), 1.0, 6.0, ((0, 8), (1, 32))),
        "restype": place_ends(jax.random.randint(key_list[3], (N,), 0, RES_TYPES), jax.random.fold_in(key_list[3], 1), 0, RES_TYPES - 1).astype(jnp.int32),
        "chain": jnp.searchsorted(jnp.cumsum(uneven(key_list[4], CHAINS, N, N // 2, 0)), jnp.arange(N), side="right").astype(jnp.int32),
        "keymask": draw_keymask(jax.random.fold_in(key_list[20], 71), 0),
        "restype_table": scatter_about(key_list[6], (RES_TYPES, D), 0.5, 3.0),
        "norm_gain": jnp.clip(1.0 + 0.15 * jax.random.normal(key_list[7], (D,), jnp.float32), 0.25, 1.75),
        "pair_gain": jnp.clip(1.0 + 0.15 * jax.random.normal(key_list[8], (CZ,), jnp.float32), 0.25, 1.75),
        "trans_gain": jnp.clip(1.0 + 0.15 * jax.random.normal(key_list[9], (D,), jnp.float32), 0.25, 1.75),
        "w_query": scatter_about(key_list[10], (D, D), D ** -0.5, 0.21875),
        "w_key": scatter_about(key_list[11], (D, D), D ** -0.5, 0.21875),
        "w_value": scatter_about(key_list[12], (D, D), D ** -0.5, 0.21875),
        "w_out": scatter_about(key_list[13], (D, D), D ** -0.5, 0.21875),
        "w_pair": scatter_about(key_list[14], (CZ, H), CZ ** -0.5, 0.5),
        "chain_weight": draw_chain_weight(jax.random.fold_in(key_list[20], 71), 0),
        "w_hidden_gate": scatter_about(key_list[16], (D, FF), D ** -0.5, 0.21875),
        "w_hidden_up": scatter_about(key_list[17], (D, FF), D ** -0.5, 0.21875),
        "w_down": scatter_about(key_list[18], (FF, D), FF ** -0.5, 0.15625),
        "cotangent": scatter_about(key_list[19], (COPIES, N, D), 1.0, 6.0, ((0, 32), (1, 8))),
    }


epsilon = 1e-05
highest_precision = lax.Precision.HIGHEST

def layer_forward(values, scales):
    average = lax.optimization_barrier(jnp.mean(values, axis=-1, keepdims=True))
    centred = values - average
    inverse = lax.rsqrt(lax.optimization_barrier(jnp.mean(centred * centred, axis=-1, keepdims=True)) + epsilon)
    normed = centred * inverse
    return (normed * scales, normed, inverse)

def layer_backward(upstream, scales, normed, inverse):
    scaled = upstream * scales
    first_moment = lax.optimization_barrier(jnp.mean(scaled, axis=-1, keepdims=True))
    second_moment = lax.optimization_barrier(jnp.mean(scaled * normed, axis=-1, keepdims=True))
    return inverse * (scaled - first_moment - normed * second_moment)

def widen(values):
    return lax.optimization_barrier(values).astype(jnp.float32)

def matmul(left, right):
    return jnp.dot(left, right, preferred_element_type=jnp.float32)

def reference(noisy, single, pair, restype, chain, keymask, restype_table, norm_gain, pair_gain, trans_gain, w_query, w_key, w_value, w_out, w_pair, chain_weight, w_hidden_gate, w_hidden_up, w_down, cotangent):
    scale = HD ** (-0.5)
    res_onehot = (restype[:, None] == jnp.arange(RES_TYPES, dtype=jnp.int32)[None, :]).astype(jnp.bfloat16)
    condition = single.astype(jnp.float32) + matmul(res_onehot, restype_table)
    pair_scaled, pair_hat, pair_inverse = layer_forward(pair.astype(jnp.float32), pair_gain)
    pair_rounded = widen(pair_scaled.astype(jnp.bfloat16))
    bias = jnp.einsum('ijc,ch->hij', pair_rounded, w_pair.astype(jnp.float32), precision=highest_precision).astype(jnp.bfloat16)
    chain_onehot = (chain[:, None] == jnp.arange(CHAINS, dtype=jnp.int32)[None, :]).astype(jnp.float32)
    key_weight = jnp.dot(chain_onehot, chain_weight, precision=highest_precision)
    same_chain = (chain[:, None] == chain[None, :]).astype(jnp.float32)
    extra = widen(bias) + same_chain[None, :, :] * key_weight.T[:, None, :]
    valid = (keymask > 0)[None, None, :]

    def one_copy(carry, pieces):
        single_sum, bias_sum, query_sum, key_sum, value_sum, out_sum = carry
        noisy_copy, upstream = pieces
        noisy_f = noisy_copy.astype(jnp.float32)
        normed_scaled, noisy_hat, noisy_inverse = layer_forward(noisy_f, norm_gain)
        inputs_x = (normed_scaled + condition).astype(jnp.bfloat16)
        query = matmul(inputs_x, w_query).astype(jnp.bfloat16)
        keys = matmul(inputs_x, w_key).astype(jnp.bfloat16)
        values = matmul(inputs_x, w_value).astype(jnp.bfloat16)
        query_heads = widen(query).reshape(N, H, HD)
        key_heads = widen(keys).reshape(N, H, HD)
        value_heads = widen(values).reshape(N, H, HD)
        logits = jnp.einsum('ihd,jhd->hij', query_heads, key_heads, precision=highest_precision) * scale + extra
        logits = jnp.where(valid, logits, -1e+30)
        highest = lax.optimization_barrier(jnp.max(logits, axis=-1, keepdims=True))
        exponent = jnp.exp(logits - highest)
        weights = exponent / lax.optimization_barrier(jnp.sum(exponent, axis=-1, keepdims=True))
        weights_b = widen(weights.astype(jnp.bfloat16))
        attended = jnp.einsum('hij,jhd->ihd', weights_b, value_heads, precision=highest_precision).reshape(N, D).astype(jnp.bfloat16)
        residual = noisy_f + matmul(attended, w_out)
        trans_scaled, trans_hat, trans_inverse = layer_forward(residual, trans_gain)
        trans_in = trans_scaled.astype(jnp.bfloat16)
        gate = matmul(trans_in, w_hidden_gate)
        up_part = matmul(trans_in, w_hidden_up)
        sigmoid_gate = jax.nn.sigmoid(gate)
        d_hidden = matmul(upstream, w_down.T)
        d_gate = (d_hidden * up_part * sigmoid_gate * (1.0 + gate * (1.0 - sigmoid_gate))).astype(jnp.bfloat16)
        d_up = (d_hidden * gate * sigmoid_gate).astype(jnp.bfloat16)
        d_trans = matmul(d_gate, w_hidden_gate.T) + matmul(d_up, w_hidden_up.T)
        d_res = upstream.astype(jnp.float32) + layer_backward(d_trans, trans_gain, trans_hat, trans_inverse)
        d_res_b = d_res.astype(jnp.bfloat16)
        out_term = matmul(attended.T, d_res_b)
        d_att = matmul(d_res_b, w_out.T).astype(jnp.bfloat16)
        d_att_heads = widen(d_att).reshape(N, H, HD)
        d_weights = jnp.einsum('ihd,jhd->hij', d_att_heads, value_heads, precision=highest_precision)
        delta = lax.optimization_barrier(jnp.sum(weights * d_weights, axis=-1, keepdims=True))
        d_logits = weights * (d_weights - delta)
        d_logits_b = widen(d_logits.astype(jnp.bfloat16))
        d_query = (jnp.einsum('hij,jhd->ihd', d_logits_b, key_heads, precision=highest_precision) * scale).reshape(N, D).astype(jnp.bfloat16)
        d_key = (jnp.einsum('hij,ihd->jhd', d_logits_b, query_heads, precision=highest_precision) * scale).reshape(N, D).astype(jnp.bfloat16)
        d_value = jnp.einsum('hij,ihd->jhd', weights_b, d_att_heads, precision=highest_precision).reshape(N, D).astype(jnp.bfloat16)
        d_inputs = matmul(d_query, w_query.T) + matmul(d_key, w_key.T) + matmul(d_value, w_value.T)
        grad_copy = (d_res + layer_backward(d_inputs, norm_gain, noisy_hat, noisy_inverse)).astype(jnp.bfloat16)
        carry = (single_sum + d_inputs, bias_sum + d_logits, query_sum + matmul(inputs_x.T, d_query), key_sum + matmul(inputs_x.T, d_key), value_sum + matmul(inputs_x.T, d_value), out_sum + out_term)
        return (carry, grad_copy)
    start = (jnp.zeros((N, D), jnp.float32), jnp.zeros((H, N, N), jnp.float32), jnp.zeros((D, D), jnp.float32), jnp.zeros((D, D), jnp.float32), jnp.zeros((D, D), jnp.float32), jnp.zeros((D, D), jnp.float32))
    carry, grad_noisy = lax.scan(one_copy, start, (noisy, cotangent))
    grad_single, bias_grad, grad_query, grad_key, grad_value, grad_out = carry
    d_pair_scaled = jnp.einsum('hij,ch->ijc', bias_grad, w_pair.astype(jnp.float32), precision=highest_precision)
    grad_pair = layer_backward(d_pair_scaled, pair_gain, pair_hat, pair_inverse).astype(jnp.bfloat16)
    grad_pair_weight = jnp.einsum('ijc,hij->ch', pair_rounded, bias_grad, precision=highest_precision)
    return (grad_noisy, grad_single, grad_pair, grad_query, grad_key, grad_value, grad_out, grad_pair_weight)
```

```python
import jax
import jax.numpy as jnp
from jax import lax
from jax.experimental import pallas as pl
from jax.experimental.pallas import tpu as pltpu
from jax.sharding import Mesh
from jax.sharding import PartitionSpec as P

TOK = ("tok_0", "tok_1")
COPY = ("copy_0", "copy_1", "copy_2")
MESH = pl.DeviceIdType.MESH
VM = pl.BlockSpec(memory_space=pltpu.VMEM)
BF = jnp.bfloat16
F32 = jnp.float32
epsilon = 1e-05


def dot(a, b, ca=1, cb=0):
    return lax.dot_general(a, b, (((ca,), (cb,)), ((), ())), preferred_element_type=F32)


class Place:
    def __init__(self):
        self.y = lax.axis_index("copy_0")
        self.z = lax.axis_index("copy_1")
        self.core = lax.axis_index("copy_2")
        self.zh = lax.axis_index("tok_0")
        self.x = lax.axis_index("tok_1")
        self.tok = self.zh * 4 + self.x
        self.chip = self.y * 4 + self.z
        self.copy = self.chip * 2 + self.core

    def around_y(self, d):
        return {"copy_0": lax.rem(self.y + d, 4)}

    def around_z(self, d):
        return {"copy_1": lax.rem(self.z + d, 4)}

    def around_x(self, d):
        return {"tok_1": lax.rem(self.x + d, 4)}

    def other_core(self):
        return {"copy_2": 1 - self.core}

    def other_half(self):
        return {"tok_0": 1 - self.zh}

    def tok_at(self, d):
        t = lax.rem(self.tok + d, 8)
        return t, {"tok_0": t // 4, "tok_1": lax.rem(t, 4)}


class Wire:
    def __init__(self, send, recv):
        self.send, self.recv, self.at, self.open = send, recv, 0, []

    def go(self, src, dst, device):
        c = pltpu.make_async_remote_copy(
            src_ref=src,
            dst_ref=dst,
            send_sem=self.send.at[self.at],
            recv_sem=self.recv.at[self.at],
            device_id=device,
            device_id_type=MESH,
        )
        self.at += 1
        c.start()
        self.open.append(c)
        return c

    def close(self):
        for c in self.open:
            c.wait_send()


def greet(devices, more=0):
    barrier = pltpu.get_barrier_semaphore()
    for d in devices:
        pl.semaphore_signal(barrier, inc=1, device_id=d, device_id_type=MESH)
    pl.semaphore_wait(barrier, len(devices) + more)


def gather_tok(w, me, src, out, rows):
    half = rows // 2
    zc = w.go(src, out.at[me.tok], me.other_half())

    def ring_start(unit_src, slot):
        left = w.go(unit_src, out.at[slot], me.around_x(3))
        right = w.go(unit_src, out.at[slot], me.around_x(1))
        return left, right

    def ring_pass(pair, zh):
        left, right = pair
        from_left = zh * 4 + lax.rem(me.x + 3, 4)
        from_right = zh * 4 + lax.rem(me.x + 1, 4)
        right.wait_recv()
        a = w.go(
            out.at[from_left, pl.ds(0, half)], out.at[from_left, pl.ds(0, half)], me.around_x(1)
        )
        left.wait_recv()
        b = w.go(
            out.at[from_right, pl.ds(half, half)],
            out.at[from_right, pl.ds(half, half)],
            me.around_x(3),
        )
        return a, b

    own = ring_start(src, me.tok)
    own_far = ring_pass(own, me.zh)
    zc.wait_recv()
    oz = 1 - me.zh
    far_slot = oz * 4 + me.x
    far = ring_start(out.at[far_slot], far_slot)
    far_far = ring_pass(far, oz)
    return own_far + far_far


def add_into(dst, a, b):
    dst[...] = (a[...].astype(F32) + b[...].astype(F32)).astype(dst.dtype)


def scatter_sum(w, me, s, near_a, near_b, from_l, from_r, from_z):
    opp = lax.rem(me.y + 2, 4) * 4
    lo = lax.rem(me.y + 3, 4) * 4
    hi = lax.rem(me.y + 1, 4) * 4
    a = w.go(s.at[pl.ds(opp, 2)], near_a, me.around_y(3))
    b = w.go(s.at[pl.ds(opp + 2, 2)], near_b, me.around_y(1))
    a.wait_recv()
    add_into(s.at[pl.ds(lo, 2)], s.at[pl.ds(lo, 2)], near_a)
    c = w.go(s.at[pl.ds(lo, 4)], from_r, me.around_y(3))
    b.wait_recv()
    add_into(s.at[pl.ds(hi + 2, 2)], s.at[pl.ds(hi + 2, 2)], near_b)
    d = w.go(s.at[pl.ds(hi, 4)], from_l, me.around_y(1))
    c.wait_recv()
    d.wait_recv()
    own = s.at[pl.ds(me.y * 4, 4)]
    own[...] = (
        own[...].astype(F32) + from_l[...].astype(F32) + from_r[...].astype(F32)
    ).astype(own.dtype)
    zs = []
    for k in (1, 2, 3):
        zt = lax.rem(me.z + k, 4)
        zs.append(w.go(s.at[me.y * 4 + zt], from_z.at[k - 1], me.around_z(k)))
    for k in zs:
        k.wait_recv()
    total = s[me.chip].astype(F32)
    for k in range(3):
        total = total + from_z[k].astype(F32)
    return total


def scatter_scratch(rest):
    return [
        pltpu.VMEM((2, *rest), BF),
        pltpu.VMEM((2, *rest), BF),
        pltpu.VMEM((4, *rest), BF),
        pltpu.VMEM((4, *rest), BF),
        pltpu.VMEM((3, *rest), BF),
    ]


def sems(n):
    return [pltpu.SemaphoreType.DMA((n,)), pltpu.SemaphoreType.DMA((n,))]


def comm_call(kernel, outs, scratch, cid, args):
    return pl.pallas_call(
        kernel,
        out_shape=outs,
        in_specs=[VM] * len(args),
        out_specs=[VM] * len(outs),
        scratch_shapes=scratch,
        compiler_params=pltpu.CompilerParams(
            collective_id=cid, has_side_effects=True, vmem_limit_bytes=48 << 20
        ),
    )(*args)


def spread_kernel(x, bt, xf, f, send, recv):
    me = Place()
    w = Wire(send, recv)
    toks = [me.tok_at(d) for d in range(1, 8)]
    greet(
        [d for _, d in toks]
        + [me.other_core()]
        + [me.around_z(k) for k in (1, 2, 3)]
        + [me.around_y(k) for k in (1, 3)]
    )
    heads = [w.go(bt.at[t], f.at[me.copy, me.tok], d) for t, d in toks]
    xf[me.tok] = x[...]
    f[me.copy, me.tok] = bt[me.tok]
    for h in heads:
        h.wait_recv()
    mine = pl.ds(4 * me.core, 4)
    theirs = pl.ds(4 * (1 - me.core), 4)
    first = w.go(f.at[me.copy, theirs], f.at[me.copy, theirs], me.other_core())
    first.wait_recv()
    last = [w.go(f.at[me.copy, mine], f.at[me.copy, mine], me.other_core())]
    chip = f.at[pl.ds(me.chip * 2, 2), mine]
    zs = [w.go(chip, chip, me.around_z(k)) for k in (1, 2, 3)]
    tail = gather_tok(w, me, x, xf, 128)
    for k, c in zip((1, 2, 3), zs):
        c.wait_recv()
        src = f.at[pl.ds((me.y * 4 + lax.rem(me.z + 4 - k, 4)) * 2, 2), mine]
        last.append(w.go(src, src, me.other_core()))
    row = f.at[pl.ds(me.y * 8, 8), mine]
    left = w.go(row, row, me.around_y(3))
    right = w.go(row, row, me.around_y(1))
    lo = lax.rem(me.y + 3, 4) * 8
    hi = lax.rem(me.y + 1, 4) * 8
    op = lax.rem(me.y + 2, 4) * 8
    right.wait_recv()
    src = f.at[pl.ds(lo, 4), mine]
    a = w.go(src, src, me.around_y(1))
    src = f.at[pl.ds(lo, 8), mine]
    last.append(w.go(src, src, me.other_core()))
    left.wait_recv()
    src = f.at[pl.ds(hi + 4, 4), mine]
    b = w.go(src, src, me.around_y(3))
    src = f.at[pl.ds(hi, 8), mine]
    last.append(w.go(src, src, me.other_core()))
    a.wait_recv()
    src = f.at[pl.ds(op, 4), mine]
    last.append(w.go(src, src, me.other_core()))
    b.wait_recv()
    src = f.at[pl.ds(op + 4, 4), mine]
    last.append(w.go(src, src, me.other_core()))
    for c in last:
        c.wait_recv()
    for c in tail:
        c.wait_recv()
    w.close()


def spread(x, bt):
    return comm_call(
        spread_kernel,
        [
            jax.ShapeDtypeStruct((8, 128, 768), BF),
            jax.ShapeDtypeStruct((32, 8, 32, 128), BF),
        ],
        sems(40),
        0,
        (x, bt),
    )


def exchange_kernel(a, o, send, recv):
    me = Place()
    w = Wire(send, recv)
    toks = [me.tok_at(d) for d in range(1, 8)]
    greet([d for _, d in toks])
    moves = [w.go(a.at[t], o.at[me.tok], d) for t, d in toks]
    o[me.tok] = a[me.tok]
    for c in moves:
        c.wait_recv()
    w.close()


def exchange(a):
    return comm_call(exchange_kernel, [jax.ShapeDtypeStruct(a.shape, BF)], sems(8), 1, (a,))[0]


def gather_kernel(a, o, send, recv):
    me = Place()
    w = Wire(send, recv)
    greet([me.other_half(), me.around_x(1), me.around_x(3)])
    o[me.tok] = a[...]
    for c in gather_tok(w, me, a, o, 768):
        c.wait_recv()
    w.close()


def gather(a):
    return comm_call(
        gather_kernel, [jax.ShapeDtypeStruct((8, *a.shape), BF)], sems(12), 2, (a,)
    )[0]


def home_kernel(
    dq, db, wg, odq, odb, owg, send, recv, db1, s1, wg1, ws, bl, bu, gt, *bufs
):
    me = Place()
    w = Wire(send, recv)
    bufs_w, bufs_d = bufs[:5], bufs[5:]
    toks = [me.tok_at(d) for d in range(1, 8)]
    turn = me.tok * 4 + lax.rem(me.copy, 4)
    turn_tok = me.copy // 4
    other = turn_tok != me.tok
    partner = {
        "copy_0": turn // 8,
        "copy_1": lax.rem(turn // 2, 4),
        "copy_2": lax.rem(turn, 2),
        "tok_0": turn_tok // 4,
        "tok_1": lax.rem(turn_tok, 4),
    }
    barrier = pltpu.get_barrier_semaphore()

    @pl.when(other)
    def _():
        pl.semaphore_signal(barrier, inc=1, device_id=partner, device_id_type=MESH)

    greet(
        [d for _, d in toks]
        + [me.other_core()]
        + [me.around_z(k) for k in (1, 2, 3)]
        + [me.around_y(k) for k in (1, 3)],
        jnp.where(other, 1, 0),
    )
    mine = pl.ds(4 * me.core, 4)
    theirs = pl.ds(4 * (1 - me.core), 4)
    cw = w.go(wg.at[1 - me.core], wg1, me.other_core())
    cb = w.go(db.at[:, :, theirs], db1, me.other_core())
    moves = [w.go(dq.at[t], odq.at[:, me.tok], d) for t, d in toks]
    odq[:, me.tok] = dq[me.tok]
    cw.wait_recv()
    ws[...] = (wg[me.core].astype(F32) + wg1[...].astype(F32)).astype(BF)
    cb.wait_recv()

    @pl.loop(0, 16)
    def _(c):
        s1[c] = (db[c, :, mine].astype(F32) + db1[c].astype(F32)).astype(BF)

    total = scatter_sum(w, me, ws, *bufs_w)
    gt[...] = total.astype(BF)
    owg[3] = gt[3]
    k = w.at
    w.at += 1

    def turned():
        return pltpu.make_async_remote_copy(
            src_ref=gt.at[pl.ds(0, 3)],
            dst_ref=owg.at[pl.ds(0, 3)],
            send_sem=send.at[k],
            recv_sem=recv.at[k],
            device_id=partner,
            device_id_type=MESH,
        )

    @pl.when(other)
    def _():
        turned().start()

    @pl.when(jnp.logical_not(other))
    def _():
        owg[pl.ds(0, 3)] = gt[pl.ds(0, 3)]

    total = scatter_sum(w, me, s1, *bufs_d)
    bu[...] = total.astype(BF)
    back = w.go(bu.at[1 - me.core], bl.at[mine], me.other_core())
    bl[mine] = bu[me.core]
    back.wait_recv()
    fan = [w.go(bl.at[t], odb.at[me.tok], d) for t, d in toks]
    odb[me.tok] = bl[me.tok]
    for c in moves + fan:
        c.wait_recv()

    @pl.when(other)
    def _():
        turned().wait()

    w.close()


def home(dq, db, wg):
    return comm_call(
        home_kernel,
        [
            jax.ShapeDtypeStruct((3, 8, 96, 128), BF),
            jax.ShapeDtypeStruct((8, 32, 128), BF),
            jax.ShapeDtypeStruct((4, 24, 128), BF),
        ],
        sems(40)
        + [
            pltpu.VMEM((16, 2, 4, 32, 128), BF),
            pltpu.VMEM((16, 2, 4, 32, 128), BF),
            pltpu.VMEM((16, 4, 24, 128), BF),
            pltpu.VMEM((16, 4, 24, 128), BF),
            pltpu.VMEM((8, 32, 128), BF),
            pltpu.VMEM((2, 4, 32, 128), BF),
            pltpu.VMEM((4, 24, 128), BF),
        ]
        + scatter_scratch((4, 24, 128))
        + scatter_scratch((2, 4, 32, 128)),
        3,
        (dq, db, wg),
    )


def finish_kernel(gs, pw, ogs, opw, send, recv, gs1, ss, p0, p1, p2, p3, r0, r1, r2, r3, *bufs):
    me = Place()
    w = Wire(send, recv)
    toks = [me.tok_at(d) for d in range(1, 8)]
    greet(
        [d for _, d in toks]
        + [me.other_core()]
        + [me.around_z(k) for k in (1, 2, 3)]
        + [me.around_y(k) for k in (1, 2, 3)]
    )
    cg = w.go(gs.at[1 - me.core], gs1, me.other_core())
    c0 = w.go(pw, r0, me.other_core())
    c0.wait_recv()
    p0[...] = pw[...] + r0[...]
    zs = [w.go(p0, r1.at[k - 1], me.around_z(k)) for k in (1, 2, 3)]
    cg.wait_recv()
    ss[...] = (gs[me.core].astype(F32) + gs1[...].astype(F32)).astype(BF)
    for c in zs:
        c.wait_recv()
    z = me.z

    def in_order(own, got, at):
        terms = []
        for k in range(4):
            d = lax.rem(at + 4 - k, 4)
            term = jnp.where(d == 0, own[...], jnp.zeros_like(own[...]))
            for j in (1, 2, 3):
                term = jnp.where(d == j, got[j - 1], term)
            terms.append(term)
        return (terms[0] + terms[1]) + (terms[2] + terms[3])

    p1[...] = in_order(p0, r1, z)
    ys = [w.go(p1, r2.at[k - 1], me.around_y(k)) for k in (1, 2, 3)]
    for c in ys:
        c.wait_recv()
    p2[...] = in_order(p1, r2, me.y)
    ts = [w.go(p2, r3.at[me.tok], d) for _, d in toks]
    r3[me.tok] = p2[...]
    ogs[...] = scatter_sum(w, me, ss, *bufs)
    for c in ts:
        c.wait_recv()
    total = r3[0]
    for k in range(1, 8):
        total = total + r3[k]
    opw[...] = total
    w.close()


def finish(gs, pw):
    return comm_call(
        finish_kernel,
        [jax.ShapeDtypeStruct((24, 128), F32), jax.ShapeDtypeStruct((8, 128), F32)],
        sems(32)
        + [
            pltpu.VMEM((16, 24, 128), BF),
            pltpu.VMEM((16, 24, 128), BF),
            pltpu.VMEM((8, 128), F32),
            pltpu.VMEM((8, 128), F32),
            pltpu.VMEM((8, 128), F32),
            pltpu.VMEM((8, 128), F32),
            pltpu.VMEM((8, 128), F32),
            pltpu.VMEM((3, 8, 128), F32),
            pltpu.VMEM((3, 8, 128), F32),
            pltpu.VMEM((8, 8, 128), F32),
        ]
        + scatter_scratch((24, 128)),
        4,
        (gs, pw),
    )


def forward_kernel(
    xf, wq, wk, wv, f, same, diff, chj, chi, att, pt, q, k, v, ab, bb, cb, vt
):
    h = lax.axis_index("tok_0") * 4 + lax.axis_index("tok_1")
    row = lax.broadcasted_iota(jnp.int32, (768, 128), 0)
    col = lax.broadcasted_iota(jnp.int32, (768, 128), 1)
    pick = jnp.where((row == col + h * 96) & (col < 96), 1.0, 0.0).astype(BF)
    ws = [dot(m[...], pick).astype(BF) for m in (wq, wk, wv)]
    for t in range(8):
        xt = xf[t]
        for m, o in zip(ws, (q, k, v)):
            o[t * 128 : (t + 1) * 128] = dot(xt, m).astype(BF)
    vt[...] = v[...].T
    ab[...] = jnp.broadcast_to(same[...], (1024, 128))
    bb[...] = jnp.broadcast_to(diff[...], (1024, 128))
    cb[...] = jnp.broadcast_to(chj[...], (1024, 128))
    scale = 96**-0.5

    @pl.loop(0, 8)
    def _(t):
        rows = pl.ds(pl.multiple_of(t * 128, 128), 128)
        s = dot(k[...], q[rows], 1, 1)
        bias = f[:, t].reshape(1024, 128).astype(F32)
        s = s * scale + (bias + jnp.where(cb[...] == chi[t], ab[...], bb[...]))
        e = jnp.exp(s - jnp.max(s, axis=0, keepdims=True))
        p = (e * (1.0 / jnp.sum(e, axis=0, keepdims=True))).astype(BF)
        pt[t] = p
        att[t] = dot(vt[...], p)[:96].astype(BF)


def forward(xf, wq, wk, wv, f, same, diff, chj, chi):
    args = (xf, wq, wk, wv, f, same, diff, chj, chi)
    return pl.pallas_call(
        forward_kernel,
        out_shape=[
            jax.ShapeDtypeStruct((8, 96, 128), BF),
            jax.ShapeDtypeStruct((8, 1024, 128), BF),
            jax.ShapeDtypeStruct((1024, 128), BF),
            jax.ShapeDtypeStruct((1024, 128), BF),
            jax.ShapeDtypeStruct((1024, 128), BF),
        ],
        in_specs=[VM] * len(args),
        out_specs=[VM] * 5,
        scratch_shapes=[
            pltpu.VMEM((1024, 128), F32),
            pltpu.VMEM((1024, 128), F32),
            pltpu.VMEM((1024, 128), jnp.int32),
            pltpu.VMEM((128, 1024), BF),
        ],
        compiler_params=pltpu.CompilerParams(vmem_limit_bytes=48 << 20),
    )(*args)


def backward_kernel(
    xf, q, k, v, pt, dr, att, wo, dq, db, wg, kt, dk, dv, go, z
):
    kt[...] = k[...].T
    dk[...] = jnp.zeros_like(dk)
    dv[...] = jnp.zeros_like(dv)
    go[...] = jnp.zeros_like(go)
    scale = 96**-0.5

    @pl.loop(0, 8)
    def _(t):
        rows = pl.ds(pl.multiple_of(t * 128, 128), 128)
        d_att = dot(wo[...], dr[t])
        d_att_b = d_att.astype(BF)
        p = pt[t]
        dp = dot(v[...], d_att_b)
        pf = p.astype(F32)
        ds = pf * (dp - jnp.sum(pf * dp, axis=0, keepdims=True))
        dsb = ds.astype(BF)
        db[:, :, t] = dsb.reshape(16, 2, 32, 128)
        dqt = (dot(kt[...], dsb)[:96] * scale).astype(BF)
        dq[t, 0] = dqt
        z[0:96, rows] = dqt
        dv[...] += dot(p, d_att.T.astype(BF))
        dk[...] += dot(dsb, q[rows])
        a = att[t].astype(F32).T.astype(BF)
        go[...] += dot(dr[t], a)

    dkt = (dk[...] * scale).T[:96].astype(BF)
    dvt = dv[...].T[:96].astype(BF)
    z[96:192] = dkt
    z[192:288] = dvt
    for t in range(8):
        dq[t, 1] = dkt[:, t * 128 : (t + 1) * 128]
        dq[t, 2] = dvt[:, t * 128 : (t + 1) * 128]
    wg[...] = jnp.zeros_like(wg)
    for s in range(3):
        r = dot(z[s * 96 : (s + 1) * 96], xf[...].reshape(1024, 768))
        for te in range(8):
            part = r[:, te * 96 : (te + 1) * 96].astype(BF)
            for j in range(4):
                wg[j % 2, 2 * te + j // 2, s, :, 0:96] = part[j * 24 : (j + 1) * 24]
    for c in range(32):
        wg[c % 2, c // 2, 3, :, 0:96] = go[c * 24 : (c + 1) * 24].astype(BF)


def backward(xf, q, k, v, pt, dr, att, wo):
    args = (xf, q, k, v, pt, dr, att, wo)
    return pl.pallas_call(
        backward_kernel,
        out_shape=[
            jax.ShapeDtypeStruct((8, 3, 96, 128), BF),
            jax.ShapeDtypeStruct((16, 2, 8, 32, 128), BF),
            jax.ShapeDtypeStruct((2, 16, 4, 24, 128), BF),
        ],
        in_specs=[VM] * len(args),
        out_specs=[VM] * 3,
        scratch_shapes=[
            pltpu.VMEM((128, 1024), BF),
            pltpu.VMEM((1024, 128), F32),
            pltpu.VMEM((1024, 128), F32),
            pltpu.VMEM((768, 96), F32),
            pltpu.VMEM((288, 1024), BF),
        ],
        compiler_params=pltpu.CompilerParams(vmem_limit_bytes=48 << 20),
    )(*args)


def layer_forward(values, scales):
    average = jnp.mean(values, axis=-1, keepdims=True)
    centred = values - average
    inverse = lax.rsqrt(jnp.mean(centred * centred, axis=-1, keepdims=True) + epsilon)
    normed = centred * inverse
    return (normed * scales, normed, inverse)


def layer_backward(upstream, scales, normed, inverse):
    scaled = upstream * scales
    first_moment = jnp.mean(scaled, axis=-1, keepdims=True)
    second_moment = jnp.mean(scaled * normed, axis=-1, keepdims=True)
    return inverse * (scaled - first_moment - normed * second_moment)


def per_device(
    noisy,
    single,
    pair,
    restype,
    chain,
    keymask,
    restype_table,
    norm_gain,
    pair_gain,
    trans_gain,
    w_query,
    w_key,
    w_value,
    w_out,
    w_pair,
    chain_weight,
    w_hidden_gate,
    w_hidden_up,
    w_down,
    cotangent,
):
    head = lax.axis_index(TOK)
    res_onehot = (restype[:, None] == jnp.arange(32, dtype=jnp.int32)[None, :]).astype(BF)
    condition = single.astype(F32) + dot(res_onehot, restype_table)
    noisy_f = noisy[0].astype(F32)
    normed_scaled, noisy_hat, noisy_inverse = layer_forward(noisy_f, norm_gain)
    x = (normed_scaled + condition).astype(BF)
    pair_t = jnp.transpose(pair, (1, 0, 2))
    pair_scaled, pair_hat, pair_inverse = layer_forward(pair_t.astype(F32), pair_gain)
    pair_rounded = pair_scaled.astype(BF)
    bias = jnp.einsum("jic,ch->hji", pair_rounded, w_pair, preferred_element_type=F32).astype(BF)
    xf, f = spread(x, bias)

    own_weight = lax.dynamic_slice_in_dim(chain_weight, head, 1, 1)
    key_weight = jnp.zeros((1024, 1), F32)
    for c in range(6):
        key_weight = jnp.where(chain[:, None] == c, own_weight[c : c + 1], key_weight)
    valid = (keymask > 0)[:, None]
    same = jnp.where(valid, key_weight, -1e30)
    diff = jnp.where(valid, jnp.zeros((1024, 1), F32), -1e30)
    att, pt, q, k, v = forward(
        xf, w_query, w_key, w_value, f, same, diff, chain[:, None], chain.reshape(8, 1, 128)
    )
    attended = exchange(att).reshape(768, 128)

    residual = noisy_f + dot(attended, w_out, 0, 0)
    trans_scaled, trans_hat, trans_inverse = layer_forward(residual, trans_gain)
    trans_in = trans_scaled.astype(BF)
    gate = dot(trans_in, w_hidden_gate)
    up_part = dot(trans_in, w_hidden_up)
    sigmoid_gate = jax.nn.sigmoid(gate)
    upstream = cotangent[0]
    d_hidden = dot(upstream, w_down, 1, 1)
    d_gate = (d_hidden * up_part * sigmoid_gate * (1.0 + gate * (1.0 - sigmoid_gate))).astype(BF)
    d_up = (d_hidden * gate * sigmoid_gate).astype(BF)
    d_trans = dot(d_gate, w_hidden_gate, 1, 1) + dot(d_up, w_hidden_up, 1, 1)
    d_res = upstream.astype(F32) + layer_backward(d_trans, trans_gain, trans_hat, trans_inverse)
    dr = gather(d_res.T.astype(BF))

    wo = jnp.pad(lax.dynamic_slice_in_dim(w_out, head * 96, 96, 0), ((0, 32), (0, 0)))
    dq, db, wg = backward(xf, q, k, v, pt, dr, att, wo)
    odq, odb, owg = home(dq, db, wg)

    odq = odq.reshape(3, 768, 128)
    d_in_t = dot(w_query, odq[0]) + dot(w_key, odq[1]) + dot(w_value, odq[2])
    grad_noisy = (d_res + layer_backward(d_in_t.T, norm_gain, noisy_hat, noisy_inverse)).astype(BF)
    gs = jnp.transpose(d_in_t.astype(BF).reshape(16, 2, 24, 128), (1, 0, 2, 3))
    d_pair_scaled = jnp.einsum("hji,ch->jic", odb, w_pair, preferred_element_type=F32)
    grad_pair = layer_backward(d_pair_scaled, pair_gain, pair_hat, pair_inverse).astype(BF)
    pw = jnp.einsum("hji,jic->hc", odb, pair_rounded, preferred_element_type=F32)
    ogs, opw = finish(gs, pw)
    grads = jnp.transpose(owg[:, :, :96].astype(F32), (0, 2, 1))
    return (
        grad_noisy[None],
        ogs.T,
        jnp.transpose(grad_pair, (1, 0, 2)),
        grads[0],
        grads[1],
        grads[2],
        grads[3],
        opw.T,
    )


def solution(mesh):
    torus = Mesh(
        mesh.devices.reshape(4, 4, 2, 2, 4), ("copy_0", "copy_1", "copy_2", "tok_0", "tok_1")
    )
    return jax.shard_map(
        per_device,
        mesh=torus,
        in_specs=(
            P(COPY, TOK, None),
            P(TOK, None),
            P(TOK, COPY, None),
            P(TOK),
            P(),
            P(),
            P(),
            P(),
            P(),
            P(),
            P(),
            P(),
            P(),
            P(),
            P(),
            P(),
            P(),
            P(),
            P(),
            P(COPY, TOK, None),
        ),
        out_specs=(
            P(COPY, TOK, None),
            P(TOK, COPY),
            P(TOK, COPY, None),
            P(TOK, COPY),
            P(TOK, COPY),
            P(TOK, COPY),
            P(TOK, COPY),
            P(),
        ),
        check_vma=False,
    )
```

```python
import jax
import jax.numpy as jnp
from jax import lax
from jax.experimental import pallas as pl
from jax.experimental.pallas import tpu as pltpu
from jax.sharding import Mesh
from jax.sharding import PartitionSpec as P

TOK = ("tok_0", "tok_1")
COPY = ("copy_0", "copy_1", "copy_2")
MESH = pl.DeviceIdType.MESH
VM = pl.BlockSpec(memory_space=pltpu.VMEM)
BF = jnp.bfloat16
F32 = jnp.float32
epsilon = 1e-05


def dot(a, b, ca=1, cb=0):
    return lax.dot_general(a, b, (((ca,), (cb,)), ((), ())), preferred_element_type=F32)


class Place:
    def __init__(self):
        self.y = lax.axis_index("copy_0")
        self.z = lax.axis_index("copy_1")
        self.core = lax.axis_index("copy_2")
        self.zh = lax.axis_index("tok_0")
        self.x = lax.axis_index("tok_1")
        self.tok = self.zh * 4 + self.x
        self.chip = self.y * 4 + self.z
        self.copy = self.chip * 2 + self.core

    def around_y(self, d):
        return {"copy_0": lax.rem(self.y + d, 4)}

    def around_z(self, d):
        return {"copy_1": lax.rem(self.z + d, 4)}

    def around_x(self, d):
        return {"tok_1": lax.rem(self.x + d, 4)}

    def other_core(self):
        return {"copy_2": 1 - self.core}

    def other_half(self):
        return {"tok_0": 1 - self.zh}

    def tok_at(self, d):
        t = lax.rem(self.tok + d, 8)
        return t, {"tok_0": t // 4, "tok_1": lax.rem(t, 4)}


class Wire:
    def __init__(self, send, recv):
        self.send, self.recv, self.at, self.open = send, recv, 0, []

    def take(self, n):
        k = self.at
        self.at += n
        return k

    def copy(self, src, dst, device, k):
        return pltpu.make_async_remote_copy(
            src_ref=src,
            dst_ref=dst,
            send_sem=self.send.at[k],
            recv_sem=self.recv.at[k],
            device_id=device,
            device_id_type=MESH,
        )

    def go(self, src, dst, device):
        c = self.copy(src, dst, device, self.take(1))
        c.start()
        self.open.append(c)
        return c

    def close(self):
        for c in self.open:
            c.wait_send()


def turns(*chains):
    chains = list(chains)
    while chains:
        for c in list(chains):
            if next(c, 0) == 0:
                chains.remove(c)


def step(chain, n=1):
    for _ in range(n):
        next(chain, 0)


def gather_chain(w, me, src, out, rows):
    half = rows // 2
    lo = lax.rem(me.x + 3, 4)
    hi = lax.rem(me.x + 1, 4)
    far = w.go(src, out.at[me.tok], me.other_half())
    left = w.go(src, out.at[me.tok], me.around_x(3))
    right = w.go(src, out.at[me.tok], me.around_x(1))
    tail = []

    def ring_pass(left, right, zh):
        right.wait_recv()
        r = out.at[zh * 4 + lo, pl.ds(0, half)]
        tail.append(w.go(r, r, me.around_x(1)))
        left.wait_recv()
        r = out.at[zh * 4 + hi, pl.ds(half, half)]
        tail.append(w.go(r, r, me.around_x(3)))

    yield 1
    ring_pass(left, right, me.zh)
    yield 1
    far.wait_recv()
    oz = 1 - me.zh
    r = out.at[oz * 4 + me.x]
    left = w.go(r, r, me.around_x(3))
    right = w.go(r, r, me.around_x(1))
    yield 1
    for c in tail:
        c.wait_recv()
    tail.clear()
    yield 1
    ring_pass(left, right, oz)
    yield 1
    for c in tail:
        c.wait_recv()


def bias_chain(w, me, bt, f, toks):
    heads = [w.go(bt.at[t], f.at[me.copy, me.tok], d) for t, d in toks]
    f[me.copy, me.tok] = bt[me.tok]
    mine = pl.ds(4 * me.core, 4)
    theirs = pl.ds(4 * (1 - me.core), 4)
    yield 1
    for h in heads:
        h.wait_recv()
    first = w.go(f.at[me.copy, theirs], f.at[me.copy, theirs], me.other_core())
    yield 1
    first.wait_recv()
    chip = f.at[pl.ds(me.chip * 2, 2), mine]
    zs = [w.go(chip, chip, me.around_z(k)) for k in (1, 2, 3)]
    last = [w.go(f.at[me.copy, mine], f.at[me.copy, mine], me.other_core())]
    yield 1
    for c in zs:
        c.wait_recv()
    row = f.at[pl.ds(me.y * 8, 8), mine]
    left = w.go(row, row, me.around_y(3))
    right = w.go(row, row, me.around_y(1))
    for k in (1, 2, 3):
        r = f.at[pl.ds((me.y * 4 + lax.rem(me.z + 4 - k, 4)) * 2, 2), mine]
        last.append(w.go(r, r, me.other_core()))
    lo = lax.rem(me.y + 3, 4) * 8
    hi = lax.rem(me.y + 1, 4) * 8
    op = lax.rem(me.y + 2, 4) * 8
    yield 1
    right.wait_recv()
    r = f.at[pl.ds(lo, 4), mine]
    a = w.go(r, r, me.around_y(1))
    r = f.at[pl.ds(lo, 8), mine]
    last.append(w.go(r, r, me.other_core()))
    left.wait_recv()
    r = f.at[pl.ds(hi + 4, 4), mine]
    b = w.go(r, r, me.around_y(3))
    r = f.at[pl.ds(hi, 8), mine]
    last.append(w.go(r, r, me.other_core()))
    yield 1
    a.wait_recv()
    r = f.at[pl.ds(op, 4), mine]
    last.append(w.go(r, r, me.other_core()))
    b.wait_recv()
    r = f.at[pl.ds(op + 4, 4), mine]
    last.append(w.go(r, r, me.other_core()))
    for c in last:
        c.wait_recv()


def add_into(dst, a, b):
    dst[...] = (a[...].astype(F32) + b[...].astype(F32)).astype(dst.dtype)


def scatter_chain(w, me, s, bufs, done):
    near_a, near_b, from_l, from_r, from_z = bufs
    opp = lax.rem(me.y + 2, 4) * 4
    lo = lax.rem(me.y + 3, 4) * 4
    hi = lax.rem(me.y + 1, 4) * 4
    a = w.go(s.at[pl.ds(opp, 2)], near_a, me.around_y(3))
    b = w.go(s.at[pl.ds(opp + 2, 2)], near_b, me.around_y(1))
    yield 1
    a.wait_recv()
    add_into(s.at[pl.ds(lo, 2)], s.at[pl.ds(lo, 2)], near_a)
    b.wait_recv()
    add_into(s.at[pl.ds(hi + 2, 2)], s.at[pl.ds(hi + 2, 2)], near_b)
    c = w.go(s.at[pl.ds(lo, 4)], from_r, me.around_y(3))
    d = w.go(s.at[pl.ds(hi, 4)], from_l, me.around_y(1))
    yield 1
    c.wait_recv()
    d.wait_recv()
    own = s.at[pl.ds(me.y * 4, 4)]
    own[...] = (
        own[...].astype(F32) + from_l[...].astype(F32) + from_r[...].astype(F32)
    ).astype(own.dtype)
    zs = []
    for k in (1, 2, 3):
        zt = lax.rem(me.z + k, 4)
        zs.append(w.go(s.at[me.y * 4 + zt], from_z.at[k - 1], me.around_z(k)))
    yield 1
    for k in zs:
        k.wait_recv()
    total = s[me.chip].astype(F32)
    for k in range(3):
        total = total + from_z[k].astype(F32)
    done(total)


def scatter_scratch(rest):
    return [
        pltpu.VMEM((2, *rest), BF),
        pltpu.VMEM((2, *rest), BF),
        pltpu.VMEM((4, *rest), BF),
        pltpu.VMEM((4, *rest), BF),
        pltpu.VMEM((3, *rest), BF),
    ]


def layer_forward(values, scales):
    average = jnp.mean(values, axis=-1, keepdims=True)
    centred = values - average
    inverse = lax.rsqrt(jnp.mean(centred * centred, axis=-1, keepdims=True) + epsilon)
    normed = centred * inverse
    return (normed * scales, normed, inverse)


def layer_backward(upstream, scales, normed, inverse):
    scaled = upstream * scales
    first_moment = jnp.mean(scaled, axis=-1, keepdims=True)
    second_moment = jnp.mean(scaled * normed, axis=-1, keepdims=True)
    return inverse * (scaled - first_moment - normed * second_moment)


INPUTS = (
    ("noisy", "single", "pair", "restype", "chain", "keymask", "table")
    + ("ng", "pg", "tg", "wp", "cot", "cw")
    + ("wq_h", "wk_h", "wv_h", "wo_h", "wg_h", "wu_h", "wd_h")
)
OUTPUTS = ("gn", "ogs", "gp", "owg", "opw")
OUT_SHAPES = (
    ((128, 768), BF),
    ((24, 128), F32),
    ((32, 128, 128), BF),
    ((4, 24, 128), BF),
    ((8, 128), F32),
)
V = pltpu.VMEM
SCRATCH = dict(
    wq=V((768, 768), BF),
    wk=V((768, 768), BF),
    wv=V((768, 768), BF),
    wo=V((768, 768), BF),
    wgate=V((768, 1536), BF),
    wup=V((768, 1536), BF),
    wdown=V((1536, 768), BF),
    load=pltpu.SemaphoreType.DMA((7,)),
    send=pltpu.SemaphoreType.DMA((140,)),
    recv=pltpu.SemaphoreType.DMA((140,)),
    xs=V((128, 768), BF),
    xf=V((8, 128, 768), BF),
    pr=V((32, 128, 128), BF),
    bj=V((256, 128), F32),
    bt=V((8, 32, 128), BF),
    f=V((32, 8, 32, 128), BF),
    ab=V((1024, 128), F32),
    bb=V((1024, 128), F32),
    cb=V((1024, 128), F32),
    q=V((1024, 128), BF),
    k=V((1024, 128), BF),
    v=V((1024, 128), BF),
    kt=V((128, 1024), BF),
    vt=V((128, 1024), BF),
    pt=V((8, 1024, 128), BF),
    att=V((8, 96, 128), BF),
    attl=V((8, 96, 128), BF),
    dh=V((128, 1536), F32),
    dres=V((128, 768), F32),
    drs=V((768, 128), BF),
    dr=V((8, 768, 128), BF),
    dq=V((8, 3, 96, 128), BF),
    odq=V((3, 8, 96, 128), BF),
    db=V((16, 2, 8, 32, 128), BF),
    dk=V((1024, 128), F32),
    dv=V((1024, 128), F32),
    go=V((768, 96), F32),
    zz=V((288, 1024), BF),
    wg=V((2, 16, 4, 24, 128), BF),
    wg1=V((16, 4, 24, 128), BF),
    ws=V((16, 4, 24, 128), BF),
    gt=V((4, 24, 128), BF),
    db1=V((16, 2, 4, 32, 128), BF),
    s1=V((16, 2, 4, 32, 128), BF),
    bu=V((2, 4, 32, 128), BF),
    bl=V((8, 32, 128), BF),
    odb=V((8, 32, 128), BF),
    gj=V((256, 128), F32),
    gs=V((2, 16, 24, 128), BF),
    gs1=V((16, 24, 128), BF),
    ss=V((16, 24, 128), BF),
    p0=V((8, 128), F32),
    p1=V((8, 128), F32),
    p2=V((8, 128), F32),
    p3=V((8, 128), F32),
    r0=V((8, 128), F32),
    r1=V((3, 8, 128), F32),
    r2=V((3, 8, 128), F32),
    r3=V((8, 8, 128), F32),
)
for name, rest in (("bw", (4, 24, 128)), ("bd", (2, 4, 32, 128)), ("bg", (24, 128))):
    for at, ref in enumerate(scatter_scratch(rest)):
        SCRATCH[name + str(at)] = ref


class Refs:
    pass


def block_kernel(*refs):
    r = Refs()
    for name, ref in zip(INPUTS + OUTPUTS + tuple(SCRATCH), refs):
        setattr(r, name, ref)
    me = Place()
    w = Wire(r.send, r.recv)
    h = me.tok
    scale = 96**-0.5
    toks = [me.tok_at(d) for d in range(1, 8)]
    turn = me.tok * 4 + lax.rem(me.copy, 4)
    turn_tok = me.copy // 4
    other = turn_tok != me.tok
    partner = {
        "copy_0": turn // 8,
        "copy_1": lax.rem(turn // 2, 4),
        "copy_2": lax.rem(turn, 2),
        "tok_0": turn_tok // 4,
        "tok_1": lax.rem(turn_tok, 4),
    }

    barrier = pltpu.get_barrier_semaphore()
    peers = [d for _, d in toks] + [me.other_core()]
    peers += [me.around_z(k) for k in (1, 2, 3)] + [me.around_y(k) for k in (1, 2, 3)]
    for d in peers:
        pl.semaphore_signal(barrier, inc=1, device_id=d, device_id_type=MESH)

    @pl.when(other)
    def _():
        pl.semaphore_signal(barrier, inc=1, device_id=partner, device_id_type=MESH)

    pairs = (
        (r.wq_h, r.wq),
        (r.wk_h, r.wk),
        (r.wv_h, r.wv),
        (r.wd_h, r.wdown),
        (r.wo_h, r.wo),
        (r.wg_h, r.wgate),
        (r.wu_h, r.wup),
    )
    loads = [pltpu.make_async_copy(a, b, r.load.at[n]) for n, (a, b) in enumerate(pairs)]
    for c in loads:
        c.start()

    noisy_f = r.noisy[...].astype(F32)
    classes = lax.broadcasted_iota(jnp.int32, (32, 128), 0) == r.restype[...]
    classes = jnp.where(classes, 1.0, 0.0).astype(BF)
    condition = r.single[...].astype(F32) + dot(classes, r.table[...], 0, 0)
    x = (layer_forward(noisy_f, r.ng[...])[0] + condition).astype(BF)
    r.xs[...] = x
    r.xf[me.tok] = x
    pl.semaphore_wait(barrier, len(peers) + jnp.where(other, 1, 0))
    xs = gather_chain(w, me, r.xs, r.xf, 128)
    step(xs)

    @pl.loop(0, 32)
    def _(j):
        p = layer_forward(r.pair[j].astype(F32), r.pg[...])[0].astype(BF)
        r.pr[j] = p
        r.bj[pl.ds(pl.multiple_of(j * 8, 8), 8)] = dot(r.wp[...], p, 1, 1)

    for n in range(8):
        r.bt[n] = r.bj[pl.ds(n, 32, stride=8)].astype(BF)
    bs = bias_chain(w, me, r.bt, r.f, toks)
    step(bs)
    step(xs)
    for t in range(8):
        code = jnp.where(r.keymask[t : t + 1] > 0, r.chain[t : t + 1], r.chain[t : t + 1] + 8)
        code = jnp.broadcast_to(code.astype(F32), (128, 128)).T
        rows = pl.ds(t * 128, 128)
        r.cb[rows] = code
        same = jnp.zeros((128, 128), F32)
        for c in range(6):
            same = jnp.where(code == c, r.cw[c, h], same)
        r.ab[rows] = same
        r.bb[rows] = jnp.where(code >= 8, -1e30, 0.0)
    step(bs)
    for c in loads[:3]:
        c.wait()
    row = lax.broadcasted_iota(jnp.int32, (768, 128), 0)
    col = lax.broadcasted_iota(jnp.int32, (768, 128), 1)
    pick = jnp.where((row == col + h * 96) & (col < 96), 1.0, 0.0).astype(BF)
    heads = [dot(m[...], pick).astype(BF) for m in (r.wq, r.wk, r.wv)]

    def project(t):
        rows = pl.ds(pl.multiple_of(t * 128, 128), 128)
        for m, o in zip(heads, (r.q, r.k, r.v)):
            o[rows] = dot(r.xf[t], m).astype(BF)

    step(bs)
    step(xs)
    loads[3].wait()
    r.dh[...] = dot(r.cot[...], r.wdown[...], 1, 1)
    step(xs)
    step(bs)
    for t in range(4):
        project(me.zh * 4 + t)
    step(xs)
    step(bs)
    step(xs)
    for t in range(4):
        project((1 - me.zh) * 4 + t)
    r.vt[...] = r.v[...].T
    r.kt[...] = r.k[...].T
    turns(bs, xs)

    ak = w.take(7)

    def att_copy(s, t):
        device = {"tok_0": t // 4, "tok_1": lax.rem(t, 4)}
        return w.copy(r.att.at[t], r.attl.at[me.tok], device, ak + s)

    @pl.loop(0, 8)
    def _(s):
        t = lax.rem(me.tok + 1 + s, 8)

        @pl.when(s > 0)
        def _():
            att_copy(s - 1, lax.rem(me.tok + s, 8)).start()

        rows = pl.ds(pl.multiple_of(t * 128, 128), 128)
        a = dot(r.k[...], r.q[rows], 1, 1)
        bias = r.f[:, t].reshape(1024, 128).astype(F32)
        own = r.chain[pl.ds(t, 1)].astype(F32)
        a = a * scale + (bias + jnp.where(r.cb[...] == own, r.ab[...], r.bb[...]))
        e = jnp.exp(a - jnp.max(a, axis=0, keepdims=True))
        p = (e * (1.0 / jnp.sum(e, axis=0, keepdims=True))).astype(BF)
        r.pt[t] = p
        r.att[t] = dot(r.vt[...], p)[:96].astype(BF)

    r.attl[me.tok] = r.att[me.tok]
    for s in range(7):
        att_copy(s, toks[s][0]).wait()

    for c in loads[4:]:
        c.wait()
    residual = noisy_f + dot(r.attl[...].reshape(768, 128), r.wo[...], 0, 0)
    scaled, trans_hat, trans_inverse = layer_forward(residual, r.tg[...])
    trans_in = scaled.astype(BF)
    d_trans = jnp.zeros((128, 768), F32)
    for n in range(3):
        cols = pl.ds(n * 512, 512)
        gate = dot(trans_in, r.wgate[:, cols])
        up = dot(trans_in, r.wup[:, cols])
        d_hidden = r.dh[:, cols]
        sig = 1.0 / (1.0 + jnp.exp(-gate))
        d_gate = (d_hidden * up * sig * (1.0 + gate * (1.0 - sig))).astype(BF)
        d_up = (d_hidden * gate * sig).astype(BF)
        d_trans = d_trans + dot(d_gate, r.wgate[:, cols], 1, 1) + dot(d_up, r.wup[:, cols], 1, 1)
    d_res = r.cot[...].astype(F32) + layer_backward(d_trans, r.tg[...], trans_hat, trans_inverse)
    r.dres[...] = d_res
    d_res_t = d_res.T.astype(BF)
    r.drs[...] = d_res_t
    r.dr[me.tok] = d_res_t
    r.dk[...] = jnp.zeros_like(r.dk)
    r.dv[...] = jnp.zeros_like(r.dv)
    r.go[...] = jnp.zeros_like(r.go)
    r.wg[...] = jnp.zeros_like(r.wg)
    ds = gather_chain(w, me, r.drs, r.dr, 768)
    wo_own = r.wo[pl.ds(pl.multiple_of(h * 96, 96), 96)]

    def back(t):
        rows = pl.ds(pl.multiple_of(t * 128, 128), 128)
        d_att = dot(wo_own, r.dr[t]).astype(BF)
        d_att = jnp.concatenate([d_att, jnp.zeros((32, 128), BF)], axis=0)
        p = r.pt[t]
        dp = dot(r.v[...], d_att)
        pf = p.astype(F32)
        dsb = (pf * (dp - jnp.sum(pf * dp, axis=0, keepdims=True))).astype(BF)
        r.db[:, :, t] = dsb.reshape(16, 2, 32, 128)
        dqt = (dot(r.kt[...], dsb)[:96] * scale).astype(BF)
        r.dq[t, 0] = dqt
        r.zz[0:96, rows] = dqt
        r.dv[...] += dot(p, d_att.astype(F32).T.astype(BF))
        r.dk[...] += dot(dsb, r.q[rows])

    turns(ds)

    @pl.loop(0, 8)
    def _(t):
        back(t)

    mine = pl.ds(4 * me.core, 4)
    theirs = pl.ds(4 * (1 - me.core), 4)

    def bias_sum():
        c = w.go(r.db.at[:, :, theirs], r.db1, me.other_core())
        yield 1
        c.wait_recv()

        @pl.loop(0, 16)
        def _(n):
            r.s1[n] = (r.db[n, :, mine].astype(F32) + r.db1[n].astype(F32)).astype(BF)

        def done(total):
            r.bu[...] = total.astype(BF)

        yield from scatter_chain(w, me, r.s1, [getattr(r, "bd" + str(n)) for n in range(5)], done)
        c = w.go(r.bu.at[1 - me.core], r.bl.at[mine], me.other_core())
        r.bl[mine] = r.bu[me.core]
        yield 1
        c.wait_recv()
        fan = [w.go(r.bl.at[t], r.odb.at[me.tok], d) for t, d in toks]
        r.odb[me.tok] = r.bl[me.tok]
        yield 1
        for c in fan:
            c.wait_recv()

    bsum = bias_sum()
    step(bsum)
    dkt = (r.dk[...] * scale).T[:96].astype(BF)
    dvt = r.dv[...].T[:96].astype(BF)
    for t in range(8):
        r.dq[t, 1] = dkt[:, t * 128 : (t + 1) * 128]
        r.dq[t, 2] = dvt[:, t * 128 : (t + 1) * 128]
    r.zz[96:192] = dkt
    r.zz[192:288] = dvt
    step(bsum)
    moves = [w.go(r.dq.at[t], r.odq.at[:, me.tok], d) for t, d in toks]
    r.odq[:, me.tok] = r.dq[me.tok]

    @pl.loop(0, 8)
    def _(t):
        r.go[...] += dot(r.dr[t], r.att[t].astype(F32).T.astype(BF))

    for n in range(32):
        r.wg[n % 2, n // 2, 3, :, 0:96] = r.go[n * 24 : (n + 1) * 24].astype(BF)
    step(bsum)
    xf = r.xf[...].reshape(1024, 768)
    for s in range(3):
        g = dot(r.zz[s * 96 : (s + 1) * 96], xf)
        for te in range(8):
            part = g[:, te * 96 : (te + 1) * 96].astype(BF)
            for j in range(4):
                r.wg[j % 2, 2 * te + j // 2, s, :, 0:96] = part[j * 24 : (j + 1) * 24]
    step(bsum)
    tk = w.take(1)

    def turned():
        return w.copy(r.gt.at[pl.ds(0, 3)], r.owg.at[pl.ds(0, 3)], partner, tk)

    def weight_sum():
        c = w.go(r.wg.at[1 - me.core], r.wg1, me.other_core())
        yield 1
        c.wait_recv()
        r.ws[...] = (r.wg[me.core].astype(F32) + r.wg1[...].astype(F32)).astype(BF)

        def done(total):
            r.gt[...] = total.astype(BF)

        yield from scatter_chain(w, me, r.ws, [getattr(r, "bw" + str(n)) for n in range(5)], done)
        r.owg[3] = r.gt[3]

        @pl.when(other)
        def _():
            turned().start()

        @pl.when(jnp.logical_not(other))
        def _():
            r.owg[pl.ds(0, 3)] = r.gt[pl.ds(0, 3)]

    wsum = weight_sum()
    step(wsum)
    step(bsum)
    for c in moves:
        c.wait_recv()
    odq = r.odq[...].reshape(3, 768, 128)
    d_in_t = dot(r.wq[...], odq[0]) + dot(r.wk[...], odq[1]) + dot(r.wv[...], odq[2])
    for n in range(32):
        r.gs[n % 2, n // 2] = d_in_t[n * 24 : (n + 1) * 24].astype(BF)

    def single_sum():
        c = w.go(r.gs.at[1 - me.core], r.gs1, me.other_core())
        yield 1
        c.wait_recv()
        r.ss[...] = (r.gs[me.core].astype(F32) + r.gs1[...].astype(F32)).astype(BF)

        def done(total):
            r.ogs[...] = total

        yield from scatter_chain(w, me, r.ss, [getattr(r, "bg" + str(n)) for n in range(5)], done)

    gsum = single_sum()
    step(wsum)
    step(gsum)
    step(bsum)
    scaled, noisy_hat, noisy_inverse = layer_forward(r.noisy[...].astype(F32), r.ng[...])
    r.gn[...] = (
        r.dres[...] + layer_backward(d_in_t.T, r.ng[...], noisy_hat, noisy_inverse)
    ).astype(BF)
    turns(bsum, wsum, gsum)

    for n in range(8):
        r.gj[pl.ds(n, 32, stride=8)] = r.odb[n].astype(F32)
    r.p3[...] = jnp.zeros_like(r.p3)

    @pl.loop(0, 32)
    def _(j):
        g = r.gj[pl.ds(pl.multiple_of(j * 8, 8), 8)].astype(BF)
        r.p3[...] += dot(g, r.pr[j])

    def in_order(own, got, at):
        terms = []
        for k in range(4):
            d = lax.rem(at + 4 - k, 4)
            term = jnp.where(d == 0, own[...], jnp.zeros_like(own[...]))
            for j in (1, 2, 3):
                term = jnp.where(d == j, got[j - 1], term)
            terms.append(term)
        return (terms[0] + terms[1]) + (terms[2] + terms[3])

    def pair_weight_sum():
        c = w.go(r.p3, r.r0, me.other_core())
        yield 1
        c.wait_recv()
        r.p0[...] = r.p3[...] + r.r0[...]
        zs = [w.go(r.p0, r.r1.at[k - 1], me.around_z(k)) for k in (1, 2, 3)]
        yield 1
        for c in zs:
            c.wait_recv()
        r.p1[...] = in_order(r.p0, r.r1, me.z)
        ys = [w.go(r.p1, r.r2.at[k - 1], me.around_y(k)) for k in (1, 2, 3)]
        yield 1
        for c in ys:
            c.wait_recv()
        r.p2[...] = in_order(r.p1, r.r2, me.y)
        ts = [w.go(r.p2, r.r3.at[me.tok], d) for _, d in toks]
        r.r3[me.tok] = r.p2[...]
        yield 1
        for c in ts:
            c.wait_recv()
        total = r.r3[0]
        for k in range(1, 8):
            total = total + r.r3[k]
        r.opw[...] = total

    psum = pair_weight_sum()
    for n in range(4):
        step(psum)

        @pl.loop(n * 8, n * 8 + 8)
        def _(j):
            g = r.gj[pl.ds(pl.multiple_of(j * 8, 8), 8)].astype(BF)
            up = dot(g, r.wp[...], 0, 0)
            hat, inverse = layer_forward(r.pair[j].astype(F32), r.pg[...])[1:]
            r.gp[j] = layer_backward(up, r.pg[...], hat, inverse).astype(BF)

    turns(psum)

    @pl.when(other)
    def _():
        turned().wait()

    w.close()


def whole_block(*args):
    spaces = [VM] * 12 + [pl.BlockSpec(memory_space=pltpu.SMEM)]
    spaces += [pl.BlockSpec(memory_space=pl.ANY)] * 7
    return pl.pallas_call(
        block_kernel,
        out_shape=[jax.ShapeDtypeStruct(s, d) for s, d in OUT_SHAPES],
        in_specs=spaces,
        out_specs=[VM] * len(OUT_SHAPES),
        scratch_shapes=list(SCRATCH.values()),
        compiler_params=pltpu.CompilerParams(
            collective_id=0, has_side_effects=True, vmem_limit_bytes=62 << 20
        ),
    )(*args)


def per_device(
    noisy,
    single,
    pair,
    restype,
    chain,
    keymask,
    restype_table,
    norm_gain,
    pair_gain,
    trans_gain,
    w_query,
    w_key,
    w_value,
    w_out,
    w_pair,
    chain_weight,
    w_hidden_gate,
    w_hidden_up,
    w_down,
    cotangent,
):
    gn, ogs, gp, owg, opw = whole_block(
        noisy[0],
        single,
        jnp.transpose(pair, (1, 0, 2)),
        restype.reshape(1, 128),
        chain.reshape(8, 128),
        keymask.reshape(8, 128),
        restype_table,
        norm_gain.reshape(1, 768),
        pair_gain.reshape(1, 128),
        trans_gain.reshape(1, 768),
        w_pair.T,
        cotangent[0],
        chain_weight,
        w_query,
        w_key,
        w_value,
        w_out,
        w_hidden_gate,
        w_hidden_up,
        w_down,
    )
    grads = jnp.transpose(owg[:, :, :96].astype(F32), (0, 2, 1))
    return (
        gn[None],
        ogs.T,
        jnp.transpose(gp, (1, 0, 2)),
        grads[0],
        grads[1],
        grads[2],
        grads[3],
        opw.T,
    )


def solution(mesh):
    torus = Mesh(
        mesh.devices.reshape(4, 4, 2, 2, 4), ("copy_0", "copy_1", "copy_2", "tok_0", "tok_1")
    )
    return jax.shard_map(
        per_device,
        mesh=torus,
        in_specs=(
            P(COPY, TOK, None),
            P(TOK, None),
            P(TOK, COPY, None),
            P(TOK),
            P(),
            P(),
            P(),
            P(),
            P(),
            P(),
            P(),
            P(),
            P(),
            P(),
            P(),
            P(),
            P(),
            P(),
            P(),
            P(COPY, TOK, None),
        ),
        out_specs=(
            P(COPY, TOK, None),
            P(TOK, COPY),
            P(TOK, COPY, None),
            P(TOK, COPY),
            P(TOK, COPY),
            P(TOK, COPY),
            P(TOK, COPY),
            P(),
        ),
        check_vma=False,
    )
```

```python
import jax
import jax.numpy as jnp
from jax import lax
from jax.experimental import pallas as pl
from jax.experimental.pallas import tpu as pltpu
from jax.sharding import Mesh
from jax.sharding import PartitionSpec as P

TOK = ("tok_0", "tok_1")
COPY = ("copy_0", "copy_1", "copy_2")
MESH = pl.DeviceIdType.MESH
VM = pl.BlockSpec(memory_space=pltpu.VMEM)
BF = jnp.bfloat16
F32 = jnp.float32
epsilon = 1e-05


def dot(a, b, ca=1, cb=0):
    return lax.dot_general(a, b, (((ca,), (cb,)), ((), ())), preferred_element_type=F32)


class Place:
    def __init__(self):
        self.y = lax.axis_index("copy_0")
        self.z = lax.axis_index("copy_1")
        self.core = lax.axis_index("copy_2")
        self.zh = lax.axis_index("tok_0")
        self.x = lax.axis_index("tok_1")
        self.tok = self.zh * 4 + self.x
        self.chip = self.y * 4 + self.z
        self.copy = self.chip * 2 + self.core

    def around_y(self, d):
        return {"copy_0": lax.rem(self.y + d, 4)}

    def around_z(self, d):
        return {"copy_1": lax.rem(self.z + d, 4)}

    def around_x(self, d):
        return {"tok_1": lax.rem(self.x + d, 4)}

    def other_core(self):
        return {"copy_2": 1 - self.core}

    def other_half(self):
        return {"tok_0": 1 - self.zh}

    def tok_at(self, d):
        t = lax.rem(self.tok + d, 8)
        return t, {"tok_0": t // 4, "tok_1": lax.rem(t, 4)}


class Wire:
    def __init__(self, send, recv):
        self.send, self.recv, self.at, self.open = send, recv, 0, []

    def take(self, n):
        k = self.at
        self.at += n
        return k

    def copy(self, src, dst, device, k):
        return pltpu.make_async_remote_copy(
            src_ref=src,
            dst_ref=dst,
            send_sem=self.send.at[k],
            recv_sem=self.recv.at[k],
            device_id=device,
            device_id_type=MESH,
        )

    def go(self, src, dst, device):
        c = self.copy(src, dst, device, self.take(1))
        c.start()
        self.open.append(c)
        return c

    def close(self):
        for c in self.open:
            c.wait_send()


def turns(*chains):
    chains = list(chains)
    while chains:
        for c in list(chains):
            if next(c, 0) == 0:
                chains.remove(c)


def step(chain, n=1):
    for _ in range(n):
        next(chain, 0)


def gather_chain(w, me, src, out, rows):
    half = rows // 2
    lo = lax.rem(me.x + 3, 4)
    hi = lax.rem(me.x + 1, 4)
    far = w.go(src, out.at[me.tok], me.other_half())
    left = w.go(src, out.at[me.tok], me.around_x(3))
    right = w.go(src, out.at[me.tok], me.around_x(1))
    tail = []

    def ring_pass(left, right, zh):
        right.wait_recv()
        r = out.at[zh * 4 + lo, pl.ds(0, half)]
        tail.append(w.go(r, r, me.around_x(1)))
        left.wait_recv()
        r = out.at[zh * 4 + hi, pl.ds(half, half)]
        tail.append(w.go(r, r, me.around_x(3)))

    yield 1
    ring_pass(left, right, me.zh)
    yield 1
    far.wait_recv()
    oz = 1 - me.zh
    r = out.at[oz * 4 + me.x]
    left = w.go(r, r, me.around_x(3))
    right = w.go(r, r, me.around_x(1))
    yield 1
    for c in tail:
        c.wait_recv()
    tail.clear()
    yield 1
    ring_pass(left, right, oz)
    yield 1
    for c in tail:
        c.wait_recv()


def bias_chain(w, me, bt, f, toks):
    heads = [w.go(bt.at[t], f.at[me.copy, me.tok], d) for t, d in toks]
    f[me.copy, me.tok] = bt[me.tok]
    mine = pl.ds(4 * me.core, 4)
    theirs = pl.ds(4 * (1 - me.core), 4)
    yield 1
    for h in heads:
        h.wait_recv()
    first = w.go(f.at[me.copy, theirs], f.at[me.copy, theirs], me.other_core())
    yield 1
    first.wait_recv()

    def part(y, k):
        return f.at[pl.ds((y * 4 + lax.rem(me.z + 4 - k, 4)) * 2, 2), mine]

    def both_ways(k):
        p = part(me.y, k)
        return w.go(p, p, me.around_y(3)), w.go(p, p, me.around_y(1))

    def to_core(p):
        last.append(w.go(p, p, me.other_core()))

    chip = part(me.y, 0)
    zs = [w.go(chip, chip, me.around_z(k)) for k in (1, 2, 3)]
    rings = [both_ways(0)]
    last = [w.go(f.at[me.copy, mine], f.at[me.copy, mine], me.other_core())]
    lo = lax.rem(me.y + 3, 4)
    hi = lax.rem(me.y + 1, 4)
    op = lax.rem(me.y + 2, 4)
    far = []
    for k in range(4):
        yield 1
        if k < 3:
            zs[k].wait_recv()
            rings.append(both_ways(k + 1))
            to_core(part(me.y, k + 1))
        yield 1
        left, right = rings[k]
        right.wait_recv()
        left.wait_recv()
        if k % 2 == 0:
            p = part(lo, k)
            far.append(w.go(p, p, me.around_y(1)))
        else:
            p = part(hi, k)
            far.append(w.go(p, p, me.around_y(3)))
        to_core(part(lo, k))
        to_core(part(hi, k))
    yield 1
    for k in range(4):
        far[k].wait_recv()
        to_core(part(op, k))
    yield 1
    for c in last:
        c.wait_recv()


def add_into(dst, a, b):
    dst[...] = (a[...].astype(F32) + b[...].astype(F32)).astype(dst.dtype)


def scatter_chain(w, me, s, bufs, done):
    near_a, near_b, from_l, from_r, from_z = bufs
    opp = lax.rem(me.y + 2, 4) * 4
    lo = lax.rem(me.y + 3, 4) * 4
    hi = lax.rem(me.y + 1, 4) * 4
    a = w.go(s.at[pl.ds(opp, 2)], near_a, me.around_y(3))
    b = w.go(s.at[pl.ds(opp + 2, 2)], near_b, me.around_y(1))
    yield 1
    a.wait_recv()
    add_into(s.at[pl.ds(lo, 2)], s.at[pl.ds(lo, 2)], near_a)
    b.wait_recv()
    add_into(s.at[pl.ds(hi + 2, 2)], s.at[pl.ds(hi + 2, 2)], near_b)
    c = w.go(s.at[pl.ds(lo, 4)], from_r, me.around_y(3))
    d = w.go(s.at[pl.ds(hi, 4)], from_l, me.around_y(1))
    yield 1
    c.wait_recv()
    d.wait_recv()
    own = s.at[pl.ds(me.y * 4, 4)]
    own[...] = (
        own[...].astype(F32) + from_l[...].astype(F32) + from_r[...].astype(F32)
    ).astype(own.dtype)
    zs = []
    for k in (1, 2, 3):
        zt = lax.rem(me.z + k, 4)
        zs.append(w.go(s.at[me.y * 4 + zt], from_z.at[k - 1], me.around_z(k)))
    yield 1
    for k in zs:
        k.wait_recv()
    total = s[me.chip].astype(F32)
    for k in range(3):
        total = total + from_z[k].astype(F32)
    done(total)


def scatter_scratch(rest):
    return [
        pltpu.VMEM((2, *rest), BF),
        pltpu.VMEM((2, *rest), BF),
        pltpu.VMEM((4, *rest), BF),
        pltpu.VMEM((4, *rest), BF),
        pltpu.VMEM((3, *rest), BF),
    ]


def layer_forward(values, scales):
    average = jnp.mean(values, axis=-1, keepdims=True)
    centred = values - average
    inverse = lax.rsqrt(jnp.mean(centred * centred, axis=-1, keepdims=True) + epsilon)
    normed = centred * inverse
    return (normed * scales, normed, inverse)


def layer_backward(upstream, scales, normed, inverse):
    scaled = upstream * scales
    first_moment = jnp.mean(scaled, axis=-1, keepdims=True)
    second_moment = jnp.mean(scaled * normed, axis=-1, keepdims=True)
    return inverse * (scaled - first_moment - normed * second_moment)


LOADED = ("noisy", "single", "restype", "table", "ng", "pair", "pg", "wp", "chain", "keymask")
LOADED += ("wq", "wk", "wv", "cot", "wdown", "wo", "tg", "wgate", "wup")
INPUTS = tuple(n + "_h" for n in LOADED) + ("cw",)
OUTPUTS = ("gn", "ogs", "gp", "owg", "opw")
OUT_SHAPES = (
    ((128, 768), BF),
    ((24, 128), F32),
    ((128, 32, 128), BF),
    ((4, 24, 128), BF),
    ((8, 128), F32),
)
V = pltpu.VMEM
SCRATCH = dict(
    wq=V((768, 768), BF),
    wk=V((768, 768), BF),
    wv=V((768, 768), BF),
    wo=V((768, 768), BF),
    wgate=V((768, 1536), BF),
    wup=V((768, 1536), BF),
    wdown=V((1536, 768), BF),
    noisy=V((128, 768), BF),
    single=V((128, 768), BF),
    restype=V((1, 128), jnp.int32),
    table=V((32, 768), BF),
    ng=V((768,), F32),
    pair=V((128, 32, 128), BF),
    pg=V((1, 128), F32),
    wp=V((8, 128), BF),
    chain=V((8, 128), jnp.int32),
    keymask=V((8, 128), jnp.int32),
    cot=V((128, 768), BF),
    tg=V((768,), F32),
    pairs=V((32 * 136, 128), F32),
    das=V((8, 96, 128), BF),
    dat=V((8, 96, 128), BF),
    g2=V((8, 4096), F32),
    load=pltpu.SemaphoreType.DMA((19,)),
    send=pltpu.SemaphoreType.DMA((180,)),
    recv=pltpu.SemaphoreType.DMA((180,)),
    xs=V((128, 768), BF),
    xf=V((8, 128, 768), BF),
    pr=V((32, 128, 128), BF),
    bj=V((256, 128), F32),
    bt=V((8, 32, 128), BF),
    f=V((32, 8, 32, 128), BF),
    ab=V((1024, 128), F32),
    bb=V((1024, 128), F32),
    cb=V((1024, 128), F32),
    q=V((1024, 128), BF),
    k=V((1024, 128), BF),
    v=V((1024, 128), BF),
    kt=V((128, 1024), BF),
    vt=V((128, 1024), BF),
    pt=V((8, 1024, 128), BF),
    att=V((8, 96, 128), BF),
    attl=V((8, 96, 128), BF),
    dh=V((128, 1536), F32),
    dres=V((128, 768), F32),
    drs=V((768, 128), BF),
    dr=V((8, 768, 128), BF),
    dq=V((8, 3, 96, 128), BF),
    odq=V((3, 8, 96, 128), BF),
    db=V((16, 2, 8, 32, 128), BF),
    dk=V((1024, 128), F32),
    dv=V((1024, 128), F32),
    go=V((768, 96), F32),
    zz=V((288, 1024), BF),
    wg=V((2, 16, 4, 24, 128), BF),
    wg1=V((16, 4, 24, 128), BF),
    ws=V((16, 4, 24, 128), BF),
    gt=V((4, 24, 128), BF),
    db1=V((16, 2, 4, 32, 128), BF),
    s1=V((16, 2, 4, 32, 128), BF),
    bu=V((2, 4, 32, 128), BF),
    bl=V((8, 32, 128), BF),
    odb=V((8, 32, 128), BF),
    gj=V((256, 128), F32),
    gs=V((2, 16, 24, 128), BF),
    gs1=V((16, 24, 128), BF),
    ss=V((16, 24, 128), BF),
    p0=V((8, 128), F32),
    p1=V((8, 128), F32),
    p2=V((8, 128), F32),
    p3=V((8, 128), F32),
    r0=V((8, 128), F32),
    r1=V((3, 8, 128), F32),
    r2=V((3, 8, 128), F32),
    r3=V((8, 8, 128), F32),
)
for name, rest in (("bw", (4, 24, 128)), ("bd", (2, 4, 32, 128)), ("bg", (24, 128))):
    for at, ref in enumerate(scatter_scratch(rest)):
        SCRATCH[name + str(at)] = ref


class Refs:
    pass


def block_kernel(*refs):
    r = Refs()
    for name, ref in zip(INPUTS + OUTPUTS + tuple(SCRATCH), refs):
        setattr(r, name, ref)
    me = Place()
    w = Wire(r.send, r.recv)
    h = me.tok
    scale = 96**-0.5
    toks = [me.tok_at(d) for d in range(1, 8)]
    turn = me.tok * 4 + lax.rem(me.copy, 4)
    turn_tok = me.copy // 4
    other = turn_tok != me.tok
    partner = {
        "copy_0": turn // 8,
        "copy_1": lax.rem(turn // 2, 4),
        "copy_2": lax.rem(turn, 2),
        "tok_0": turn_tok // 4,
        "tok_1": lax.rem(turn_tok, 4),
    }

    barrier = pltpu.get_barrier_semaphore()
    peers = [d for _, d in toks] + [me.other_core()]
    peers += [me.around_z(k) for k in (1, 2, 3)] + [me.around_y(k) for k in (1, 2, 3)]
    for d in peers:
        pl.semaphore_signal(barrier, inc=1, device_id=d, device_id_type=MESH)

    @pl.when(other)
    def _():
        pl.semaphore_signal(barrier, inc=1, device_id=partner, device_id_type=MESH)

    loads = {}
    for n, name in enumerate(LOADED):
        c = pltpu.make_async_copy(getattr(r, name + "_h"), getattr(r, name), r.load.at[n])
        c.start()
        loads[name] = c

    def ready(*names):
        for name in names:
            loads[name].wait()

    ready("noisy", "single", "restype", "table", "ng")
    gain = r.ng[...].reshape(1, 768)
    noisy_f = r.noisy[...].astype(F32)
    classes = lax.broadcasted_iota(jnp.int32, (32, 128), 0) == r.restype[...]
    classes = jnp.where(classes, 1.0, 0.0).astype(BF)
    condition = r.single[...].astype(F32) + dot(classes, r.table[...], 0, 0)
    x = (layer_forward(noisy_f, gain)[0] + condition).astype(BF)
    r.xs[...] = x
    r.xf[me.tok] = x

    ready("pair", "pg", "wp")

    @pl.loop(0, 16)
    def _(n):
        for m in range(8):
            i = n * 8 + m
            r.pairs[pl.ds(i, 32, stride=136)] = r.pair[i].astype(F32)

    def column(j):
        return pl.ds(pl.multiple_of(j * 136, 8), 128)

    @pl.loop(0, 8)
    def _(n):
        for m in range(4):
            j = n * 4 + m
            p = layer_forward(r.pairs[column(j)], r.pg[...])[0].astype(BF)
            r.pr[j] = p
            r.bj[pl.ds(pl.multiple_of(j * 8, 8), 8)] = dot(r.wp[...], p, 1, 1)

    for n in range(8):
        r.bt[n] = r.bj[pl.ds(n, 32, stride=8)].astype(BF)
    pl.semaphore_wait(barrier, len(peers) + jnp.where(other, 1, 0))
    bs = bias_chain(w, me, r.bt, r.f, toks)
    step(bs)
    xs = gather_chain(w, me, r.xs, r.xf, 128)
    step(xs)
    ready("chain", "keymask")
    for t in range(8):
        code = jnp.where(r.keymask[t : t + 1] > 0, r.chain[t : t + 1], r.chain[t : t + 1] + 8)
        code = jnp.broadcast_to(code.astype(F32), (128, 128)).T
        rows = pl.ds(t * 128, 128)
        r.cb[rows] = code
        same = jnp.zeros((128, 128), F32)
        for c in range(6):
            same = jnp.where(code == c, r.cw[c, h], same)
        r.ab[rows] = same
        r.bb[rows] = jnp.where(code >= 8, -1e30, 0.0)
    step(bs)
    ready("wq", "wk", "wv")
    row = lax.broadcasted_iota(jnp.int32, (768, 128), 0)
    col = lax.broadcasted_iota(jnp.int32, (768, 128), 1)
    pick = jnp.where((row == col + h * 96) & (col < 96), 1.0, 0.0).astype(BF)
    heads = [dot(m[...], pick).astype(BF) for m in (r.wq, r.wk, r.wv)]

    def project(t):
        rows = pl.ds(pl.multiple_of(t * 128, 128), 128)
        for m, o in zip(heads, (r.q, r.k, r.v)):
            o[rows] = dot(r.xf[t], m).astype(BF)

    step(bs)
    step(xs)
    ready("cot", "wdown")
    r.dh[...] = dot(r.cot[...], r.wdown[...], 1, 1)
    step(bs)
    step(xs)
    step(bs)
    step(xs)
    for t in range(4):
        project(me.zh * 4 + t)
    step(bs)
    step(xs)
    step(bs)
    step(xs)
    step(bs)
    for t in range(4):
        project((1 - me.zh) * 4 + t)
    step(bs)
    r.vt[...] = r.v[...].T
    r.kt[...] = r.k[...].T
    turns(bs, xs)

    ak = w.take(7)

    def att_copy(s, t):
        device = {"tok_0": t // 4, "tok_1": lax.rem(t, 4)}
        return w.copy(r.att.at[t], r.attl.at[me.tok], device, ak + s)

    @pl.loop(0, 8)
    def _(s):
        t = lax.rem(me.tok + 1 + s, 8)

        @pl.when(s > 0)
        def _():
            att_copy(s - 1, lax.rem(me.tok + s, 8)).start()

        rows = pl.ds(pl.multiple_of(t * 128, 128), 128)
        a = dot(r.k[...], r.q[rows], 1, 1)
        bias = r.f[:, t].reshape(1024, 128).astype(F32)
        own = r.chain[pl.ds(t, 1)].astype(F32)
        a = a * scale + (bias + jnp.where(r.cb[...] == own, r.ab[...], r.bb[...]))
        e = jnp.exp(a - jnp.max(a, axis=0, keepdims=True))
        p = (e * (1.0 / jnp.sum(e, axis=0, keepdims=True))).astype(BF)
        r.pt[t] = p
        r.att[t] = dot(r.vt[...], p)[:96].astype(BF)

    r.attl[me.tok] = r.att[me.tok]
    for s in range(7):
        att_copy(s, toks[s][0]).wait()

    ready("wo", "tg", "wgate", "wup")
    trans_gain = r.tg[...].reshape(1, 768)
    residual = noisy_f + dot(r.attl[...].reshape(768, 128), r.wo[...], 0, 0)
    scaled, trans_hat, trans_inverse = layer_forward(residual, trans_gain)
    trans_in = scaled.astype(BF)
    d_trans = jnp.zeros((128, 768), F32)
    for n in range(3):
        cols = pl.ds(n * 512, 512)
        gate = dot(trans_in, r.wgate[:, cols])
        up = dot(trans_in, r.wup[:, cols])
        d_hidden = r.dh[:, cols]
        sig = 1.0 / (1.0 + jnp.exp(-gate))
        d_gate = (d_hidden * up * sig * (1.0 + gate * (1.0 - sig))).astype(BF)
        d_up = (d_hidden * gate * sig).astype(BF)
        d_trans = d_trans + dot(d_gate, r.wgate[:, cols], 1, 1) + dot(d_up, r.wup[:, cols], 1, 1)
    d_res = r.cot[...].astype(F32) + layer_backward(d_trans, trans_gain, trans_hat, trans_inverse)
    r.dres[...] = d_res
    d_att = dot(r.wo[...], d_res.astype(BF), 1, 1)
    r.das[...] = d_att.astype(BF).reshape(8, 96, 128)
    d_res_t = d_res.T.astype(BF)
    r.drs[...] = d_res_t
    r.dr[me.tok] = d_res_t
    fan = [w.go(r.das.at[t], r.dat.at[me.tok], d) for t, d in toks]
    r.dat[me.tok] = r.das[me.tok]
    ds = gather_chain(w, me, r.drs, r.dr, 768)
    step(ds)
    r.dk[...] = jnp.zeros_like(r.dk)
    r.dv[...] = jnp.zeros_like(r.dv)
    r.go[...] = jnp.zeros_like(r.go)
    r.wg[...] = jnp.zeros_like(r.wg)
    for c in fan:
        c.wait_recv()

    def back(t):
        rows = pl.ds(pl.multiple_of(t * 128, 128), 128)
        d_att = jnp.concatenate([r.dat[t], jnp.zeros((32, 128), BF)], axis=0)
        p = r.pt[t]
        dp = dot(r.v[...], d_att)
        pf = p.astype(F32)
        dsb = (pf * (dp - jnp.sum(pf * dp, axis=0, keepdims=True))).astype(BF)
        r.db[:, :, t] = dsb.reshape(16, 2, 32, 128)
        dqt = (dot(r.kt[...], dsb)[:96] * scale).astype(BF)
        r.dq[t, 0] = dqt
        r.zz[0:96, rows] = dqt
        r.dv[...] += dot(p, d_att.astype(F32).T.astype(BF))
        r.dk[...] += dot(dsb, r.q[rows])


    @pl.loop(0, 4)
    def _(n):
        back(4 * (1 - me.core) + n)

    mine = pl.ds(4 * me.core, 4)
    theirs = pl.ds(4 * (1 - me.core), 4)

    def bias_sum():
        c = w.go(r.db.at[:, :, theirs], r.db1, me.other_core())
        yield 1
        c.wait_recv()

        @pl.loop(0, 16)
        def _(n):
            r.s1[n] = (r.db[n, :, mine].astype(F32) + r.db1[n].astype(F32)).astype(BF)

        def done(total):
            r.bu[...] = total.astype(BF)

        yield from scatter_chain(w, me, r.s1, [getattr(r, "bd" + str(n)) for n in range(5)], done)
        c = w.go(r.bu.at[1 - me.core], r.bl.at[mine], me.other_core())
        r.bl[mine] = r.bu[me.core]
        yield 1
        c.wait_recv()
        fan = [w.go(r.bl.at[t], r.odb.at[me.tok], d) for t, d in toks]
        r.odb[me.tok] = r.bl[me.tok]
        yield 1
        for c in fan:
            c.wait_recv()

    bsum = bias_sum()
    step(bsum)
    step(ds)

    @pl.loop(0, 4)
    def _(n):
        back(4 * me.core + n)

    step(bsum)
    step(ds)
    dkt = (r.dk[...] * scale).T[:96].astype(BF)
    dvt = r.dv[...].T[:96].astype(BF)
    for t in range(8):
        r.dq[t, 1] = dkt[:, t * 128 : (t + 1) * 128]
        r.dq[t, 2] = dvt[:, t * 128 : (t + 1) * 128]
    r.zz[96:192] = dkt
    r.zz[192:288] = dvt
    moves = [w.go(r.dq.at[t], r.odq.at[:, me.tok], d) for t, d in toks]
    r.odq[:, me.tok] = r.dq[me.tok]

    xf = r.xf[...].reshape(1024, 768)
    for s in range(3):
        g = dot(r.zz[s * 96 : (s + 1) * 96], xf)
        for te in range(8):
            part = g[:, te * 96 : (te + 1) * 96].astype(BF)
            for j in range(4):
                r.wg[j % 2, 2 * te + j // 2, s, :, 0:96] = part[j * 24 : (j + 1) * 24]
    step(bsum)
    turns(ds)

    @pl.loop(0, 8)
    def _(t):
        r.go[...] += dot(r.dr[t], r.att[t].astype(F32).T.astype(BF))

    for n in range(32):
        r.wg[n % 2, n // 2, 3, :, 0:96] = r.go[n * 24 : (n + 1) * 24].astype(BF)
    tk = w.take(1)

    def turned():
        return w.copy(r.gt.at[pl.ds(0, 3)], r.owg.at[pl.ds(0, 3)], partner, tk)

    def weight_sum():
        c = w.go(r.wg.at[1 - me.core], r.wg1, me.other_core())
        yield 1
        c.wait_recv()
        r.ws[...] = (r.wg[me.core].astype(F32) + r.wg1[...].astype(F32)).astype(BF)

        def done(total):
            r.gt[...] = total.astype(BF)

        yield from scatter_chain(w, me, r.ws, [getattr(r, "bw" + str(n)) for n in range(5)], done)
        r.owg[3] = r.gt[3]

        @pl.when(other)
        def _():
            turned().start()

        @pl.when(jnp.logical_not(other))
        def _():
            r.owg[pl.ds(0, 3)] = r.gt[pl.ds(0, 3)]

    wsum = weight_sum()
    step(wsum)
    for c in moves:
        c.wait_recv()
    odq = r.odq[...].reshape(3, 768, 128)
    d_in_t = dot(r.wq[...], odq[0]) + dot(r.wk[...], odq[1]) + dot(r.wv[...], odq[2])
    for n in range(32):
        r.gs[n % 2, n // 2] = d_in_t[n * 24 : (n + 1) * 24].astype(BF)

    def single_sum():
        c = w.go(r.gs.at[1 - me.core], r.gs1, me.other_core())
        yield 1
        c.wait_recv()
        r.ss[...] = (r.gs[me.core].astype(F32) + r.gs1[...].astype(F32)).astype(BF)

        def done(total):
            r.ogs[...] = total

        yield from scatter_chain(w, me, r.ss, [getattr(r, "bg" + str(n)) for n in range(5)], done)

    gsum = single_sum()
    step(gsum)
    step(bsum)
    step(wsum)
    step(gsum)
    scaled, noisy_hat, noisy_inverse = layer_forward(r.noisy[...].astype(F32), gain)
    r.gn[...] = (
        r.dres[...] + layer_backward(d_in_t.T, gain, noisy_hat, noisy_inverse)
    ).astype(BF)
    step(wsum)
    step(gsum)
    step(bsum)
    step(bsum)
    step(wsum)
    step(gsum)
    turns(bsum)

    for n in range(8):
        r.gj[pl.ds(n, 32, stride=8)] = r.odb[n].astype(F32)
    for n in range(32):
        r.g2[:, n * 128 : (n + 1) * 128] = r.gj[n * 8 : (n + 1) * 8]
    r.p3[...] = dot(r.g2[...].astype(BF), r.pr[...].reshape(4096, 128))

    def in_order(own, got, at):
        terms = []
        for k in range(4):
            d = lax.rem(at + 4 - k, 4)
            term = jnp.where(d == 0, own[...], jnp.zeros_like(own[...]))
            for j in (1, 2, 3):
                term = jnp.where(d == j, got[j - 1], term)
            terms.append(term)
        return (terms[0] + terms[1]) + (terms[2] + terms[3])

    def pair_weight_sum():
        c = w.go(r.p3, r.r0, me.other_core())
        yield 1
        c.wait_recv()
        r.p0[...] = r.p3[...] + r.r0[...]
        zs = [w.go(r.p0, r.r1.at[k - 1], me.around_z(k)) for k in (1, 2, 3)]
        yield 1
        for c in zs:
            c.wait_recv()
        r.p1[...] = in_order(r.p0, r.r1, me.z)
        ys = [w.go(r.p1, r.r2.at[k - 1], me.around_y(k)) for k in (1, 2, 3)]
        yield 1
        for c in ys:
            c.wait_recv()
        r.p2[...] = in_order(r.p1, r.r2, me.y)
        ts = [w.go(r.p2, r.r3.at[me.tok], d) for _, d in toks]
        r.r3[me.tok] = r.p2[...]
        yield 1
        for c in ts:
            c.wait_recv()
        total = r.r3[0]
        for k in range(1, 8):
            total = total + r.r3[k]
        r.opw[...] = total

    psum = pair_weight_sum()
    for n in range(4):
        step(psum)

        @pl.loop(n * 2, n * 2 + 2)
        def _(b):
            for m in range(4):
                j = b * 4 + m
                g = r.gj[pl.ds(pl.multiple_of(j * 8, 8), 8)].astype(BF)
                up = dot(g, r.wp[...], 0, 0)
                hat, inverse = layer_forward(r.pairs[column(j)], r.pg[...])[1:]
                r.pairs[column(j)] = layer_backward(up, r.pg[...], hat, inverse)

    @pl.loop(0, 16)
    def _(n):
        for m in range(8):
            i = n * 8 + m
            r.gp[i] = r.pairs[pl.ds(i, 32, stride=136)].astype(BF)

    turns(psum, wsum, gsum)

    @pl.when(other)
    def _():
        turned().wait()

    w.close()


def whole_block(*args):
    spaces = [pl.BlockSpec(memory_space=pl.ANY)] * len(LOADED)
    spaces += [pl.BlockSpec(memory_space=pltpu.SMEM)]
    return pl.pallas_call(
        block_kernel,
        out_shape=[jax.ShapeDtypeStruct(s, d) for s, d in OUT_SHAPES],
        in_specs=spaces,
        out_specs=[VM] * len(OUT_SHAPES),
        scratch_shapes=list(SCRATCH.values()),
        compiler_params=pltpu.CompilerParams(
            collective_id=0, has_side_effects=True, vmem_limit_bytes=62 << 20
        ),
    )(*args)


def per_device(
    noisy,
    single,
    pair,
    restype,
    chain,
    keymask,
    restype_table,
    norm_gain,
    pair_gain,
    trans_gain,
    w_query,
    w_key,
    w_value,
    w_out,
    w_pair,
    chain_weight,
    w_hidden_gate,
    w_hidden_up,
    w_down,
    cotangent,
):
    gn, ogs, gp, owg, opw = whole_block(
        noisy[0],
        single,
        restype.reshape(1, 128),
        restype_table,
        norm_gain,
        pair,
        pair_gain.reshape(1, 128),
        w_pair.T,
        chain.reshape(8, 128),
        keymask.reshape(8, 128),
        w_query,
        w_key,
        w_value,
        cotangent[0],
        w_down,
        w_out,
        trans_gain,
        w_hidden_gate,
        w_hidden_up,
        chain_weight,
    )
    grads = jnp.transpose(owg[:, :, :96].astype(F32), (0, 2, 1))
    return (
        gn[None],
        ogs.T,
        gp,
        grads[0],
        grads[1],
        grads[2],
        grads[3],
        opw.T,
    )


def solution(mesh):
    torus = Mesh(
        mesh.devices.reshape(4, 4, 2, 2, 4), ("copy_0", "copy_1", "copy_2", "tok_0", "tok_1")
    )
    return jax.shard_map(
        per_device,
        mesh=torus,
        in_specs=(
            P(COPY, TOK, None),
            P(TOK, None),
            P(TOK, COPY, None),
            P(TOK),
            P(),
            P(),
            P(),
            P(),
            P(),
            P(),
            P(),
            P(),
            P(),
            P(),
            P(),
            P(),
            P(),
            P(),
            P(),
            P(COPY, TOK, None),
        ),
        out_specs=(
            P(COPY, TOK, None),
            P(TOK, COPY),
            P(TOK, COPY, None),
            P(TOK, COPY),
            P(TOK, COPY),
            P(TOK, COPY),
            P(TOK, COPY),
            P(),
        ),
        check_vma=False,
    )
```

```python
import jax
import jax.numpy as jnp
from jax import lax
from jax.experimental import pallas as pl
from jax.experimental.pallas import tpu as pltpu
from jax.sharding import Mesh
from jax.sharding import PartitionSpec as P

TOK = ("tok_0", "tok_1")
COPY = ("copy_0", "copy_1", "copy_2")
MESH = pl.DeviceIdType.MESH
VM = pl.BlockSpec(memory_space=pltpu.VMEM)
BF = jnp.bfloat16
F32 = jnp.float32
epsilon = 1e-05


def dot(a, b, ca=1, cb=0):
    return lax.dot_general(a, b, (((ca,), (cb,)), ((), ())), preferred_element_type=F32)


class Place:
    def __init__(self):
        self.y = lax.axis_index("copy_0")
        self.z = lax.axis_index("copy_1")
        self.core = lax.axis_index("copy_2")
        self.zh = lax.axis_index("tok_0")
        self.x = lax.axis_index("tok_1")
        self.tok = self.zh * 4 + self.x
        self.chip = self.y * 4 + self.z
        self.copy = self.chip * 2 + self.core

    def around_y(self, d):
        return {"copy_0": lax.rem(self.y + d, 4)}

    def around_z(self, d):
        return {"copy_1": lax.rem(self.z + d, 4)}

    def around_x(self, d):
        return {"tok_1": lax.rem(self.x + d, 4)}

    def other_core(self):
        return {"copy_2": 1 - self.core}

    def other_half(self):
        return {"tok_0": 1 - self.zh}

    def tok_at(self, d):
        t = lax.rem(self.tok + d, 8)
        return t, {"tok_0": t // 4, "tok_1": lax.rem(t, 4)}


class Wire:
    def __init__(self, send, recv):
        self.send, self.recv, self.at, self.open = send, recv, 0, []

    def take(self, n):
        k = self.at
        self.at += n
        return k

    def copy(self, src, dst, device, k):
        return pltpu.make_async_remote_copy(
            src_ref=src,
            dst_ref=dst,
            send_sem=self.send.at[k],
            recv_sem=self.recv.at[k],
            device_id=device,
            device_id_type=MESH,
        )

    def go(self, src, dst, device):
        c = self.copy(src, dst, device, self.take(1))
        c.start()
        self.open.append(c)
        return c

    def close(self):
        for c in self.open:
            c.wait_send()


def turns(*chains):
    chains = list(chains)
    while chains:
        for c in list(chains):
            if next(c, 0) == 0:
                chains.remove(c)


def step(chain, n=1):
    for _ in range(n):
        next(chain, 0)


def gather_chain(w, me, src, out, rows):
    half = rows // 2
    lo = lax.rem(me.x + 3, 4)
    hi = lax.rem(me.x + 1, 4)
    far = w.go(src, out.at[me.tok], me.other_half())
    left = w.go(src, out.at[me.tok], me.around_x(3))
    right = w.go(src, out.at[me.tok], me.around_x(1))
    tail = []

    def ring_pass(left, right, zh):
        right.wait_recv()
        r = out.at[zh * 4 + lo, pl.ds(0, half)]
        tail.append(w.go(r, r, me.around_x(1)))
        left.wait_recv()
        r = out.at[zh * 4 + hi, pl.ds(half, half)]
        tail.append(w.go(r, r, me.around_x(3)))

    yield 1
    ring_pass(left, right, me.zh)
    yield 1
    far.wait_recv()
    oz = 1 - me.zh
    r = out.at[oz * 4 + me.x]
    left = w.go(r, r, me.around_x(3))
    right = w.go(r, r, me.around_x(1))
    yield 1
    for c in tail:
        c.wait_recv()
    tail.clear()
    yield 1
    ring_pass(left, right, oz)
    yield 1
    for c in tail:
        c.wait_recv()


def bias_chain(w, me, bt, f, toks):
    heads = [w.go(bt.at[t], f.at[me.copy, me.tok], d) for t, d in toks]
    f[me.copy, me.tok] = bt[me.tok]
    mine = pl.ds(4 * me.core, 4)
    theirs = pl.ds(4 * (1 - me.core), 4)
    yield 1
    for h in heads:
        h.wait_recv()
    first = w.go(f.at[me.copy, theirs], f.at[me.copy, theirs], me.other_core())
    yield 1
    first.wait_recv()

    def part(y, k):
        return f.at[pl.ds((y * 4 + lax.rem(me.z + 4 - k, 4)) * 2, 2), mine]

    def both_ways(k):
        p = part(me.y, k)
        return w.go(p, p, me.around_y(3)), w.go(p, p, me.around_y(1))

    def to_core(p):
        last.append(w.go(p, p, me.other_core()))

    chip = part(me.y, 0)
    zs = [w.go(chip, chip, me.around_z(k)) for k in (1, 2, 3)]
    rings = [both_ways(0)]
    last = [w.go(f.at[me.copy, mine], f.at[me.copy, mine], me.other_core())]
    lo = lax.rem(me.y + 3, 4)
    hi = lax.rem(me.y + 1, 4)
    op = lax.rem(me.y + 2, 4)
    far = []
    for k in range(4):
        yield 1
        if k < 3:
            zs[k].wait_recv()
            rings.append(both_ways(k + 1))
            to_core(part(me.y, k + 1))
        yield 1
        left, right = rings[k]
        right.wait_recv()
        left.wait_recv()
        if k % 2 == 0:
            p = part(lo, k)
            far.append(w.go(p, p, me.around_y(1)))
        else:
            p = part(hi, k)
            far.append(w.go(p, p, me.around_y(3)))
        to_core(part(lo, k))
        to_core(part(hi, k))
    yield 1
    for k in range(4):
        far[k].wait_recv()
        to_core(part(op, k))
    yield 1
    for c in last:
        c.wait_recv()


def add_into(dst, a, b):
    dst[...] = (a[...].astype(F32) + b[...].astype(F32)).astype(dst.dtype)


def scatter_chain(w, me, s, bufs, done):
    near_a, near_b, from_l, from_r, from_z = bufs
    opp = lax.rem(me.y + 2, 4) * 4
    lo = lax.rem(me.y + 3, 4) * 4
    hi = lax.rem(me.y + 1, 4) * 4
    a = w.go(s.at[pl.ds(opp, 2)], near_a, me.around_y(3))
    b = w.go(s.at[pl.ds(opp + 2, 2)], near_b, me.around_y(1))
    yield 1
    a.wait_recv()
    add_into(s.at[pl.ds(lo, 2)], s.at[pl.ds(lo, 2)], near_a)
    b.wait_recv()
    add_into(s.at[pl.ds(hi + 2, 2)], s.at[pl.ds(hi + 2, 2)], near_b)
    c = w.go(s.at[pl.ds(lo, 4)], from_r, me.around_y(3))
    d = w.go(s.at[pl.ds(hi, 4)], from_l, me.around_y(1))
    yield 1
    c.wait_recv()
    d.wait_recv()
    own = s.at[pl.ds(me.y * 4, 4)]
    own[...] = (
        own[...].astype(F32) + from_l[...].astype(F32) + from_r[...].astype(F32)
    ).astype(own.dtype)
    zs = []
    for k in (1, 2, 3):
        zt = lax.rem(me.z + k, 4)
        zs.append(w.go(s.at[me.y * 4 + zt], from_z.at[k - 1], me.around_z(k)))
    yield 1
    for k in zs:
        k.wait_recv()
    total = s[me.chip].astype(F32)
    for k in range(3):
        total = total + from_z[k].astype(F32)
    done(total)


def scatter_scratch(rest):
    return [
        pltpu.VMEM((2, *rest), BF),
        pltpu.VMEM((2, *rest), BF),
        pltpu.VMEM((4, *rest), BF),
        pltpu.VMEM((4, *rest), BF),
        pltpu.VMEM((3, *rest), BF),
    ]


def layer_forward(values, scales):
    average = jnp.mean(values, axis=-1, keepdims=True)
    centred = values - average
    inverse = lax.rsqrt(jnp.mean(centred * centred, axis=-1, keepdims=True) + epsilon)
    normed = centred * inverse
    return (normed * scales, normed, inverse)


def layer_backward(upstream, scales, normed, inverse):
    scaled = upstream * scales
    first_moment = jnp.mean(scaled, axis=-1, keepdims=True)
    second_moment = jnp.mean(scaled * normed, axis=-1, keepdims=True)
    return inverse * (scaled - first_moment - normed * second_moment)


LOADED = ("noisy", "single", "restype", "table", "ng", "pair", "pg", "wp", "chain", "keymask")
LOADED += ("wq", "wk", "wv", "cot", "wdown", "wo", "tg", "wgate", "wup")
INPUTS = tuple(n + "_h" for n in LOADED) + ("cw",)
OUTPUTS = ("gn", "ogs", "gp", "owg", "opw")
OUT_SHAPES = (
    ((128, 768), BF),
    ((2, 24, 128), F32),
    ((128, 32, 128), BF),
    ((3, 24, 128), BF),
    ((8, 128), F32),
)
V = pltpu.VMEM
SCRATCH = dict(
    wq=V((768, 768), BF),
    wk=V((768, 768), BF),
    wv=V((768, 768), BF),
    wo=V((768, 768), BF),
    wgate=V((768, 1536), BF),
    wup=V((768, 1536), BF),
    wdown=V((1536, 768), BF),
    noisy=V((128, 768), BF),
    single=V((128, 768), BF),
    restype=V((1, 128), jnp.int32),
    table=V((32, 768), BF),
    ng=V((768,), F32),
    pair=V((128, 32, 128), BF),
    pg=V((1, 128), F32),
    wp=V((8, 128), BF),
    chain=V((8, 128), jnp.int32),
    keymask=V((8, 128), jnp.int32),
    cot=V((128, 768), BF),
    tg=V((768,), F32),
    pairs=V((32 * 136, 128), F32),
    das=V((8, 96, 128), BF),
    dat=V((8, 96, 128), BF),
    g2=V((8, 4096), F32),
    load=pltpu.SemaphoreType.DMA((19,)),
    send=pltpu.SemaphoreType.DMA((180,)),
    recv=pltpu.SemaphoreType.DMA((180,)),
    xs=V((128, 768), BF),
    xf=V((8, 128, 768), BF),
    pr=V((32, 128, 128), BF),
    bj=V((256, 128), F32),
    bt=V((8, 32, 128), BF),
    f=V((32, 8, 32, 128), BF),
    ab=V((1024, 128), F32),
    bb=V((1024, 128), F32),
    cb=V((1024, 128), F32),
    q=V((1024, 128), BF),
    k=V((1024, 128), BF),
    v=V((1024, 128), BF),
    kt=V((128, 1024), BF),
    vt=V((128, 1024), BF),
    pt=V((8, 1024, 128), BF),
    att=V((8, 96, 128), BF),
    attl=V((8, 96, 128), BF),
    dh=V((128, 1536), F32),
    dres=V((128, 768), F32),
    drs=V((768, 128), BF),
    dr=V((8, 768, 128), BF),
    dq=V((8, 3, 96, 128), BF),
    odq=V((3, 8, 96, 128), BF),
    db=V((16, 2, 8, 32, 128), BF),
    dk=V((1024, 128), F32),
    dv=V((1024, 128), F32),
    go=V((768, 96), F32),
    zz=V((288, 1024), BF),
    wg=V((2, 16, 3, 24, 128), BF),
    wg1=V((16, 3, 24, 128), BF),
    ws=V((16, 3, 24, 128), BF),
    gt=V((3, 24, 128), BF),
    db1=V((16, 2, 4, 32, 128), BF),
    s1=V((16, 2, 4, 32, 128), BF),
    bu=V((2, 4, 32, 128), BF),
    bl=V((8, 32, 128), BF),
    odb=V((8, 32, 128), BF),
    gj=V((256, 128), F32),
    gs=V((2, 16, 2, 24, 128), BF),
    gs1=V((16, 2, 24, 128), BF),
    ss=V((16, 2, 24, 128), BF),
    p0=V((8, 128), F32),
    p1=V((8, 128), F32),
    p2=V((8, 128), F32),
    p3=V((8, 128), F32),
    r0=V((8, 128), F32),
    r1=V((3, 8, 128), F32),
    r2=V((3, 8, 128), F32),
    r3=V((8, 8, 128), F32),
)
for name, rest in (("bw", (3, 24, 128)), ("bd", (2, 4, 32, 128)), ("bg", (2, 24, 128))):
    for at, ref in enumerate(scatter_scratch(rest)):
        SCRATCH[name + str(at)] = ref


class Refs:
    pass


def block_kernel(*refs):
    r = Refs()
    for name, ref in zip(INPUTS + OUTPUTS + tuple(SCRATCH), refs):
        setattr(r, name, ref)
    me = Place()
    w = Wire(r.send, r.recv)
    h = me.tok
    scale = 96**-0.5
    toks = [me.tok_at(d) for d in range(1, 8)]
    turn = me.tok * 4 + lax.rem(me.copy, 4)
    turn_tok = me.copy // 4
    other = turn_tok != me.tok
    partner = {
        "copy_0": turn // 8,
        "copy_1": lax.rem(turn // 2, 4),
        "copy_2": lax.rem(turn, 2),
        "tok_0": turn_tok // 4,
        "tok_1": lax.rem(turn_tok, 4),
    }

    barrier = pltpu.get_barrier_semaphore()
    peers = [d for _, d in toks] + [me.other_core()]
    peers += [me.around_z(k) for k in (1, 2, 3)] + [me.around_y(k) for k in (1, 2, 3)]
    for d in peers:
        pl.semaphore_signal(barrier, inc=1, device_id=d, device_id_type=MESH)

    @pl.when(other)
    def _():
        pl.semaphore_signal(barrier, inc=1, device_id=partner, device_id_type=MESH)

    loads = {}
    for n, name in enumerate(LOADED):
        c = pltpu.make_async_copy(getattr(r, name + "_h"), getattr(r, name), r.load.at[n])
        c.start()
        loads[name] = c

    def ready(*names):
        for name in names:
            loads[name].wait()

    ready("noisy", "single", "restype", "table", "ng")
    gain = r.ng[...].reshape(1, 768)
    noisy_f = r.noisy[...].astype(F32)
    classes = lax.broadcasted_iota(jnp.int32, (32, 128), 0) == r.restype[...]
    classes = jnp.where(classes, 1.0, 0.0).astype(BF)
    condition = r.single[...].astype(F32) + dot(classes, r.table[...], 0, 0)
    x = (layer_forward(noisy_f, gain)[0] + condition).astype(BF)
    r.xs[...] = x
    r.xf[me.tok] = x

    ready("pair", "pg", "wp")

    @pl.loop(0, 16)
    def _(n):
        for m in range(8):
            i = n * 8 + m
            r.pairs[pl.ds(i, 32, stride=136)] = r.pair[i].astype(F32)

    def column(j):
        return pl.ds(pl.multiple_of(j * 136, 8), 128)

    @pl.loop(0, 8)
    def _(n):
        for m in range(4):
            j = n * 4 + m
            p = layer_forward(r.pairs[column(j)], r.pg[...])[0].astype(BF)
            r.pr[j] = p
            r.bj[pl.ds(pl.multiple_of(j * 8, 8), 8)] = dot(r.wp[...], p, 1, 1)

    for n in range(8):
        r.bt[n] = r.bj[pl.ds(n, 32, stride=8)].astype(BF)
    pl.semaphore_wait(barrier, len(peers) + jnp.where(other, 1, 0))
    bs = bias_chain(w, me, r.bt, r.f, toks)
    step(bs)
    xs = gather_chain(w, me, r.xs, r.xf, 128)
    step(xs)
    ready("chain", "keymask")
    for t in range(8):
        code = jnp.where(r.keymask[t : t + 1] > 0, r.chain[t : t + 1], r.chain[t : t + 1] + 8)
        code = jnp.broadcast_to(code.astype(F32), (128, 128)).T
        rows = pl.ds(t * 128, 128)
        r.cb[rows] = code
        same = jnp.zeros((128, 128), F32)
        for c in range(6):
            same = jnp.where(code == c, r.cw[c, h], same)
        r.ab[rows] = same
        r.bb[rows] = jnp.where(code >= 8, -1e30, 0.0)
    step(bs)
    ready("wq", "wk", "wv")
    row = lax.broadcasted_iota(jnp.int32, (768, 128), 0)
    col = lax.broadcasted_iota(jnp.int32, (768, 128), 1)
    pick = jnp.where((row == col + h * 96) & (col < 96), 1.0, 0.0).astype(BF)
    heads = [dot(m[...], pick).astype(BF) for m in (r.wq, r.wk, r.wv)]

    def project(t):
        rows = pl.ds(pl.multiple_of(t * 128, 128), 128)
        for m, o in zip(heads, (r.q, r.k, r.v)):
            o[rows] = dot(r.xf[t], m).astype(BF)

    step(bs)
    step(xs)
    ready("cot", "wdown")
    r.dh[...] = dot(r.cot[...], r.wdown[...], 1, 1)
    step(bs)
    step(xs)
    step(bs)
    step(xs)
    for t in range(4):
        project(me.zh * 4 + t)
    step(bs)
    step(xs)
    step(bs)
    step(xs)
    step(bs)
    for t in range(4):
        project((1 - me.zh) * 4 + t)
    step(bs)
    r.vt[...] = r.v[...].T
    r.kt[...] = r.k[...].T
    turns(bs, xs)

    ak = w.take(7)

    def att_copy(s, t):
        device = {"tok_0": t // 4, "tok_1": lax.rem(t, 4)}
        return w.copy(r.att.at[t], r.attl.at[me.tok], device, ak + s)

    @pl.loop(0, 8)
    def _(s):
        t = lax.rem(me.tok + 1 + s, 8)

        @pl.when(s > 0)
        def _():
            att_copy(s - 1, lax.rem(me.tok + s, 8)).start()

        rows = pl.ds(pl.multiple_of(t * 128, 128), 128)
        a = dot(r.k[...], r.q[rows], 1, 1)
        bias = r.f[:, t].reshape(1024, 128).astype(F32)
        own = r.chain[pl.ds(t, 1)].astype(F32)
        a = a * scale + (bias + jnp.where(r.cb[...] == own, r.ab[...], r.bb[...]))
        e = jnp.exp(a - jnp.max(a, axis=0, keepdims=True))
        p = (e * (1.0 / jnp.sum(e, axis=0, keepdims=True))).astype(BF)
        r.pt[t] = p
        r.att[t] = dot(r.vt[...], p)[:96].astype(BF)

    r.attl[me.tok] = r.att[me.tok]
    for s in range(7):
        att_copy(s, toks[s][0]).wait()

    ready("wo", "tg", "wgate", "wup")
    trans_gain = r.tg[...].reshape(1, 768)
    residual = noisy_f + dot(r.attl[...].reshape(768, 128), r.wo[...], 0, 0)
    scaled, trans_hat, trans_inverse = layer_forward(residual, trans_gain)
    trans_in = scaled.astype(BF)
    d_trans = jnp.zeros((128, 768), F32)
    for n in range(3):
        cols = pl.ds(n * 512, 512)
        gate = dot(trans_in, r.wgate[:, cols])
        up = dot(trans_in, r.wup[:, cols])
        d_hidden = r.dh[:, cols]
        sig = 1.0 / (1.0 + jnp.exp(-gate))
        d_gate = (d_hidden * up * sig * (1.0 + gate * (1.0 - sig))).astype(BF)
        d_up = (d_hidden * gate * sig).astype(BF)
        d_trans = d_trans + dot(d_gate, r.wgate[:, cols], 1, 1) + dot(d_up, r.wup[:, cols], 1, 1)
    d_res = r.cot[...].astype(F32) + layer_backward(d_trans, trans_gain, trans_hat, trans_inverse)
    r.dres[...] = d_res
    d_att = dot(r.wo[...], d_res.astype(BF), 1, 1)
    r.das[...] = d_att.astype(BF).reshape(8, 96, 128)
    d_res_t = d_res.T.astype(BF)
    r.drs[...] = d_res_t
    r.dr[me.tok] = d_res_t
    fan = [w.go(r.das.at[t], r.dat.at[me.tok], d) for t, d in toks]
    r.dat[me.tok] = r.das[me.tok]
    ds = gather_chain(w, me, r.drs, r.dr, 768)
    step(ds)
    r.dk[...] = jnp.zeros_like(r.dk)
    r.dv[...] = jnp.zeros_like(r.dv)
    r.go[...] = jnp.zeros_like(r.go)
    r.wg[...] = jnp.zeros_like(r.wg)
    r.gs[...] = jnp.zeros_like(r.gs)
    for c in fan:
        c.wait_recv()

    def back(t):
        rows = pl.ds(pl.multiple_of(t * 128, 128), 128)
        d_att = jnp.concatenate([r.dat[t], jnp.zeros((32, 128), BF)], axis=0)
        p = r.pt[t]
        dp = dot(r.v[...], d_att)
        pf = p.astype(F32)
        dsb = (pf * (dp - jnp.sum(pf * dp, axis=0, keepdims=True))).astype(BF)
        r.db[:, :, t] = dsb.reshape(16, 2, 32, 128)
        dqt = (dot(r.kt[...], dsb)[:96] * scale).astype(BF)
        r.dq[t, 0] = dqt
        r.zz[0:96, rows] = dqt
        r.dv[...] += dot(p, d_att.astype(F32).T.astype(BF))
        r.dk[...] += dot(dsb, r.q[rows])


    @pl.loop(0, 4)
    def _(n):
        back(4 * (1 - me.core) + n)

    mine = pl.ds(4 * me.core, 4)
    theirs = pl.ds(4 * (1 - me.core), 4)

    def bias_sum():
        c = w.go(r.db.at[:, :, theirs], r.db1, me.other_core())
        yield 1
        c.wait_recv()

        @pl.loop(0, 16)
        def _(n):
            r.s1[n] = (r.db[n, :, mine].astype(F32) + r.db1[n].astype(F32)).astype(BF)

        def done(total):
            r.bu[...] = total.astype(BF)

        yield from scatter_chain(w, me, r.s1, [getattr(r, "bd" + str(n)) for n in range(5)], done)
        c = w.go(r.bu.at[1 - me.core], r.bl.at[mine], me.other_core())
        r.bl[mine] = r.bu[me.core]
        yield 1
        c.wait_recv()
        fan = [w.go(r.bl.at[t], r.odb.at[me.tok], d) for t, d in toks]
        r.odb[me.tok] = r.bl[me.tok]
        yield 1
        for c in fan:
            c.wait_recv()

    bsum = bias_sum()
    step(bsum)
    step(ds)

    @pl.loop(0, 4)
    def _(n):
        back(4 * me.core + n)

    step(bsum)
    step(ds)
    dkt = (r.dk[...] * scale).T[:96].astype(BF)
    dvt = r.dv[...].T[:96].astype(BF)
    for t in range(8):
        r.dq[t, 1] = dkt[:, t * 128 : (t + 1) * 128]
        r.dq[t, 2] = dvt[:, t * 128 : (t + 1) * 128]
    r.zz[96:192] = dkt
    r.zz[192:288] = dvt
    moves = [w.go(r.dq.at[t], r.odq.at[:, me.tok], d) for t, d in toks]
    r.odq[:, me.tok] = r.dq[me.tok]

    xf = r.xf[...].reshape(1024, 768)
    for s in range(3):
        g = dot(r.zz[s * 96 : (s + 1) * 96], xf)
        for te in range(8):
            part = g[:, te * 96 : (te + 1) * 96].astype(BF)
            for j in range(4):
                r.wg[j % 2, 2 * te + j // 2, s, :, 0:96] = part[j * 24 : (j + 1) * 24]
    tk = w.take(1)

    def turned():
        return w.copy(r.gt, r.owg, partner, tk)

    def weight_sum():
        c = w.go(r.wg.at[1 - me.core], r.wg1, me.other_core())
        yield 1
        c.wait_recv()
        r.ws[...] = (r.wg[me.core].astype(F32) + r.wg1[...].astype(F32)).astype(BF)

        def done(total):
            r.gt[...] = total.astype(BF)

        yield from scatter_chain(w, me, r.ws, [getattr(r, "bw" + str(n)) for n in range(5)], done)
        @pl.when(other)
        def _():
            turned().start()

        @pl.when(jnp.logical_not(other))
        def _():
            r.owg[...] = r.gt[...]

    wsum = weight_sum()
    step(wsum)
    step(bsum)
    step(ds)
    step(wsum)
    step(ds)
    step(bsum)
    turns(ds)

    @pl.loop(0, 8)
    def _(t):
        r.go[...] += dot(r.dr[t], r.att[t].astype(F32).T.astype(BF))

    for n in range(32):
        r.gs[n % 2, n // 2, 1, :, 0:96] = r.go[n * 24 : (n + 1) * 24].astype(BF)
    step(wsum)
    step(bsum)
    for c in moves:
        c.wait_recv()
    odq = r.odq[...].reshape(3, 768, 128)
    d_in_t = dot(r.wq[...], odq[0]) + dot(r.wk[...], odq[1]) + dot(r.wv[...], odq[2])
    for n in range(32):
        r.gs[n % 2, n // 2, 0] = d_in_t[n * 24 : (n + 1) * 24].astype(BF)

    def single_sum():
        c = w.go(r.gs.at[1 - me.core], r.gs1, me.other_core())
        yield 1
        c.wait_recv()
        r.ss[...] = (r.gs[me.core].astype(F32) + r.gs1[...].astype(F32)).astype(BF)

        def done(total):
            r.ogs[...] = total

        yield from scatter_chain(w, me, r.ss, [getattr(r, "bg" + str(n)) for n in range(5)], done)

    gsum = single_sum()
    step(gsum)
    step(bsum)
    step(wsum)
    step(gsum)
    scaled, noisy_hat, noisy_inverse = layer_forward(r.noisy[...].astype(F32), gain)
    r.gn[...] = (
        r.dres[...] + layer_backward(d_in_t.T, gain, noisy_hat, noisy_inverse)
    ).astype(BF)
    step(wsum)
    step(gsum)
    turns(bsum)

    for n in range(8):
        r.gj[pl.ds(n, 32, stride=8)] = r.odb[n].astype(F32)
    for n in range(32):
        r.g2[:, n * 128 : (n + 1) * 128] = r.gj[n * 8 : (n + 1) * 8]
    r.p3[...] = dot(r.g2[...].astype(BF), r.pr[...].reshape(4096, 128))

    def in_order(own, got, at):
        terms = []
        for k in range(4):
            d = lax.rem(at + 4 - k, 4)
            term = jnp.where(d == 0, own[...], jnp.zeros_like(own[...]))
            for j in (1, 2, 3):
                term = jnp.where(d == j, got[j - 1], term)
            terms.append(term)
        return (terms[0] + terms[1]) + (terms[2] + terms[3])

    def pair_weight_sum():
        c = w.go(r.p3, r.r0, me.other_core())
        yield 1
        c.wait_recv()
        r.p0[...] = r.p3[...] + r.r0[...]
        zs = [w.go(r.p0, r.r1.at[k - 1], me.around_z(k)) for k in (1, 2, 3)]
        yield 1
        for c in zs:
            c.wait_recv()
        r.p1[...] = in_order(r.p0, r.r1, me.z)
        ys = [w.go(r.p1, r.r2.at[k - 1], me.around_y(k)) for k in (1, 2, 3)]
        yield 1
        for c in ys:
            c.wait_recv()
        r.p2[...] = in_order(r.p1, r.r2, me.y)
        ts = [w.go(r.p2, r.r3.at[me.tok], d) for _, d in toks]
        r.r3[me.tok] = r.p2[...]
        yield 1
        for c in ts:
            c.wait_recv()
        total = r.r3[0]
        for k in range(1, 8):
            total = total + r.r3[k]
        r.opw[...] = total

    psum = pair_weight_sum()
    for n in range(4):
        step(psum)
        if n in (1, 2):
            step(gsum)

        @pl.loop(n * 2, n * 2 + 2)
        def _(b):
            for m in range(4):
                j = b * 4 + m
                g = r.gj[pl.ds(pl.multiple_of(j * 8, 8), 8)].astype(BF)
                up = dot(g, r.wp[...], 0, 0)
                hat, inverse = layer_forward(r.pairs[column(j)], r.pg[...])[1:]
                r.pairs[column(j)] = layer_backward(up, r.pg[...], hat, inverse)

    @pl.loop(0, 16)
    def _(n):
        for m in range(8):
            i = n * 8 + m
            r.gp[i] = r.pairs[pl.ds(i, 32, stride=136)].astype(BF)

    turns(psum, wsum, gsum)

    @pl.when(other)
    def _():
        turned().wait()

    w.close()


def whole_block(*args):
    spaces = [pl.BlockSpec(memory_space=pl.ANY)] * len(LOADED)
    spaces += [pl.BlockSpec(memory_space=pltpu.SMEM)]
    return pl.pallas_call(
        block_kernel,
        out_shape=[jax.ShapeDtypeStruct(s, d) for s, d in OUT_SHAPES],
        in_specs=spaces,
        out_specs=[VM] * len(OUT_SHAPES),
        scratch_shapes=list(SCRATCH.values()),
        compiler_params=pltpu.CompilerParams(
            collective_id=0, has_side_effects=True, vmem_limit_bytes=62 << 20
        ),
    )(*args)


def results_kernel(gn, ogs, gp, owg, opw, *rest):
    outs, (vgn, vgp, vogs, vowg, vopw, sem) = rest[:8], rest[8:]
    ogn, osingle, ogp, oq, ok, ov, oo, opair = outs
    ins = [pltpu.make_async_copy(gp.at[pl.ds(n * 32, 32)], vgp.at[n], sem.at[n]) for n in range(4)]
    ins.append(pltpu.make_async_copy(gn, vgn, sem.at[4]))
    small = [
        pltpu.make_async_copy(a, b, sem.at[5 + n])
        for n, (a, b) in enumerate(((ogs, vogs), (owg, vowg), (opw, vopw)))
    ]
    for c in ins + small:
        c.start()
    back = [
        pltpu.make_async_copy(vgp.at[n], ogp.at[pl.ds(n * 32, 32)], sem.at[8 + n])
        for n in range(4)
    ]
    back.append(pltpu.make_async_copy(vgn, ogn, sem.at[12]))
    for a, b in zip(ins, back):
        a.wait()
        b.start()
    for c in small:
        c.wait()
    osingle[...] = vogs[0]
    for n, o in enumerate((oq, ok, ov)):
        o[...] = vowg[n, :, 0:96].astype(F32)
    oo[...] = vogs[1, :, 0:96]
    opair[...] = vopw[...]
    for c in back:
        c.wait()


def results(*args):
    grad = jax.ShapeDtypeStruct((24, 96), F32)
    anywhere = pl.BlockSpec(memory_space=pl.ANY)
    return pl.pallas_call(
        results_kernel,
        out_shape=[
            jax.ShapeDtypeStruct((128, 768), BF),
            jax.ShapeDtypeStruct((24, 128), F32),
            jax.ShapeDtypeStruct((128, 32, 128), BF),
            grad,
            grad,
            grad,
            grad,
            jax.ShapeDtypeStruct((8, 128), F32),
        ],
        in_specs=[anywhere] * 5,
        out_specs=[anywhere, VM, anywhere, VM, VM, VM, VM, VM],
        scratch_shapes=[
            V((128, 768), BF),
            V((4, 32, 32, 128), BF),
            V((2, 24, 128), F32),
            V((3, 24, 128), BF),
            V((8, 128), F32),
            pltpu.SemaphoreType.DMA((13,)),
        ],
        compiler_params=pltpu.CompilerParams(vmem_limit_bytes=60 << 20),
    )(*args)


def per_device(
    noisy,
    single,
    pair,
    restype,
    chain,
    keymask,
    restype_table,
    norm_gain,
    pair_gain,
    trans_gain,
    w_query,
    w_key,
    w_value,
    w_out,
    w_pair,
    chain_weight,
    w_hidden_gate,
    w_hidden_up,
    w_down,
    cotangent,
):
    parts = whole_block(
        noisy[0],
        single,
        restype.reshape(1, 128),
        restype_table,
        norm_gain,
        pair,
        pair_gain.reshape(1, 128),
        w_pair.T,
        chain.reshape(8, 128),
        keymask.reshape(8, 128),
        w_query,
        w_key,
        w_value,
        cotangent[0],
        w_down,
        w_out,
        trans_gain,
        w_hidden_gate,
        w_hidden_up,
        chain_weight,
    )
    gn, gsingle, gp, gq, gk, gv, gout, gpw = results(*parts)
    return gn[None], gsingle.T, gp, gq.T, gk.T, gv.T, gout.T, gpw.T


def solution(mesh):
    torus = Mesh(
        mesh.devices.reshape(4, 4, 2, 2, 4), ("copy_0", "copy_1", "copy_2", "tok_0", "tok_1")
    )
    return jax.shard_map(
        per_device,
        mesh=torus,
        in_specs=(
            P(COPY, TOK, None),
            P(TOK, None),
            P(TOK, COPY, None),
            P(TOK),
            P(),
            P(),
            P(),
            P(),
            P(),
            P(),
            P(),
            P(),
            P(),
            P(),
            P(),
            P(),
            P(),
            P(),
            P(),
            P(COPY, TOK, None),
        ),
        out_specs=(
            P(COPY, TOK, None),
            P(TOK, COPY),
            P(TOK, COPY, None),
            P(TOK, COPY),
            P(TOK, COPY),
            P(TOK, COPY),
            P(TOK, COPY),
            P(),
        ),
        check_vma=False,
    )
```

```python
import jax
import jax.numpy as jnp
from jax import lax
from jax.experimental import pallas as pl
from jax.experimental.pallas import tpu as pltpu
from jax.sharding import Mesh
from jax.sharding import PartitionSpec as P

TOK = ("tok_0", "tok_1")
COPY = ("copy_0", "copy_1", "copy_2")
MESH = pl.DeviceIdType.MESH
VM = pl.BlockSpec(memory_space=pltpu.VMEM)
BF = jnp.bfloat16
F32 = jnp.float32
epsilon = 1e-05


def dot(a, b, ca=1, cb=0):
    return lax.dot_general(a, b, (((ca,), (cb,)), ((), ())), preferred_element_type=F32)


class Place:
    def __init__(self):
        self.y = lax.axis_index("copy_0")
        self.z = lax.axis_index("copy_1")
        self.core = lax.axis_index("copy_2")
        self.zh = lax.axis_index("tok_0")
        self.x = lax.axis_index("tok_1")
        self.tok = self.zh * 4 + self.x
        self.chip = self.y * 4 + self.z
        self.copy = self.chip * 2 + self.core

    def around_y(self, d):
        return {"copy_0": lax.rem(self.y + d, 4)}

    def around_z(self, d):
        return {"copy_1": lax.rem(self.z + d, 4)}

    def around_x(self, d):
        return {"tok_1": lax.rem(self.x + d, 4)}

    def other_core(self):
        return {"copy_2": 1 - self.core}

    def other_half(self):
        return {"tok_0": 1 - self.zh}

    def tok_at(self, d):
        t = lax.rem(self.tok + d, 8)
        return t, {"tok_0": t // 4, "tok_1": lax.rem(t, 4)}


class Wire:
    def __init__(self, send, recv):
        self.send, self.recv, self.at, self.open = send, recv, 0, []

    def take(self, n):
        k = self.at
        self.at += n
        return k

    def copy(self, src, dst, device, k):
        return pltpu.make_async_remote_copy(
            src_ref=src,
            dst_ref=dst,
            send_sem=self.send.at[k],
            recv_sem=self.recv.at[k],
            device_id=device,
            device_id_type=MESH,
        )

    def go(self, src, dst, device):
        c = self.copy(src, dst, device, self.take(1))
        c.start()
        self.open.append(c)
        return c

    def close(self):
        for c in self.open:
            c.wait_send()
        self.open = []


def turns(*chains):
    chains = list(chains)
    while chains:
        for c in list(chains):
            if next(c, 0) == 0:
                chains.remove(c)


def step(chain, n=1):
    for _ in range(n):
        next(chain, 0)


def gather_chain(w, me, src, out, rows):
    half = rows // 2
    lo = lax.rem(me.x + 3, 4)
    hi = lax.rem(me.x + 1, 4)
    far = w.go(src, out.at[me.tok], me.other_half())
    left = w.go(src, out.at[me.tok], me.around_x(3))
    right = w.go(src, out.at[me.tok], me.around_x(1))
    tail = []

    def ring_pass(left, right, zh):
        right.wait_recv()
        r = out.at[zh * 4 + lo, pl.ds(0, half)]
        tail.append(w.go(r, r, me.around_x(1)))
        left.wait_recv()
        r = out.at[zh * 4 + hi, pl.ds(half, half)]
        tail.append(w.go(r, r, me.around_x(3)))

    yield 1
    ring_pass(left, right, me.zh)
    yield 1
    far.wait_recv()
    oz = 1 - me.zh
    r = out.at[oz * 4 + me.x]
    left = w.go(r, r, me.around_x(3))
    right = w.go(r, r, me.around_x(1))
    yield 1
    for c in tail:
        c.wait_recv()
    tail.clear()
    yield 1
    ring_pass(left, right, oz)
    yield 1
    for c in tail:
        c.wait_recv()


def bias_chain(w, me, bt, f, toks):
    heads = [w.go(bt.at[t], f.at[me.copy, me.tok], d) for t, d in toks]
    f[me.copy, me.tok] = bt[me.tok]
    mine = pl.ds(4 * me.core, 4)
    theirs = pl.ds(4 * (1 - me.core), 4)
    yield 1
    for h in heads:
        h.wait_recv()
    first = w.go(f.at[me.copy, theirs], f.at[me.copy, theirs], me.other_core())
    yield 1
    first.wait_recv()

    def part(y, k):
        return f.at[pl.ds((y * 4 + lax.rem(me.z + 4 - k, 4)) * 2, 2), mine]

    def both_ways(k):
        p = part(me.y, k)
        return w.go(p, p, me.around_y(3)), w.go(p, p, me.around_y(1))

    def to_core(p):
        last.append(w.go(p, p, me.other_core()))

    chip = part(me.y, 0)
    zs = [w.go(chip, chip, me.around_z(k)) for k in (1, 2, 3)]
    rings = [both_ways(0)]
    last = [w.go(f.at[me.copy, mine], f.at[me.copy, mine], me.other_core())]
    lo = lax.rem(me.y + 3, 4)
    hi = lax.rem(me.y + 1, 4)
    op = lax.rem(me.y + 2, 4)
    far = []
    for k in range(4):
        yield 1
        if k < 3:
            zs[k].wait_recv()
            rings.append(both_ways(k + 1))
            to_core(part(me.y, k + 1))
        yield 1
        left, right = rings[k]
        right.wait_recv()
        left.wait_recv()
        if k % 2 == 0:
            p = part(lo, k)
            far.append(w.go(p, p, me.around_y(1)))
        else:
            p = part(hi, k)
            far.append(w.go(p, p, me.around_y(3)))
        to_core(part(lo, k))
        to_core(part(hi, k))
    yield 1
    for k in range(4):
        far[k].wait_recv()
        to_core(part(op, k))
    yield 1
    for c in last:
        c.wait_recv()


def add_into(dst, a, b):
    dst[...] = (a[...].astype(F32) + b[...].astype(F32)).astype(dst.dtype)


def scatter_chain(w, me, s, bufs, done):
    near_a, near_b, from_l, from_r, from_z = bufs
    opp = lax.rem(me.y + 2, 4) * 4
    lo = lax.rem(me.y + 3, 4) * 4
    hi = lax.rem(me.y + 1, 4) * 4
    a = w.go(s.at[pl.ds(opp, 2)], near_a, me.around_y(3))
    b = w.go(s.at[pl.ds(opp + 2, 2)], near_b, me.around_y(1))
    yield 1
    a.wait_recv()
    add_into(s.at[pl.ds(lo, 2)], s.at[pl.ds(lo, 2)], near_a)
    b.wait_recv()
    add_into(s.at[pl.ds(hi + 2, 2)], s.at[pl.ds(hi + 2, 2)], near_b)
    c = w.go(s.at[pl.ds(lo, 4)], from_r, me.around_y(3))
    d = w.go(s.at[pl.ds(hi, 4)], from_l, me.around_y(1))
    yield 1
    c.wait_recv()
    d.wait_recv()
    own = s.at[pl.ds(me.y * 4, 4)]
    own[...] = (
        own[...].astype(F32) + from_l[...].astype(F32) + from_r[...].astype(F32)
    ).astype(own.dtype)
    zs = []
    for k in (1, 2, 3):
        zt = lax.rem(me.z + k, 4)
        zs.append(w.go(s.at[me.y * 4 + zt], from_z.at[k - 1], me.around_z(k)))
    yield 1
    for k in zs:
        k.wait_recv()
    total = s[me.chip].astype(F32)
    for k in range(3):
        total = total + from_z[k].astype(F32)
    done(total)


def scatter_scratch(rest):
    return [
        pltpu.VMEM((2, *rest), BF),
        pltpu.VMEM((2, *rest), BF),
        pltpu.VMEM((4, *rest), BF),
        pltpu.VMEM((4, *rest), BF),
        pltpu.VMEM((3, *rest), BF),
    ]


def layer_forward(values, scales):
    average = jnp.mean(values, axis=-1, keepdims=True)
    centred = values - average
    inverse = lax.rsqrt(jnp.mean(centred * centred, axis=-1, keepdims=True) + epsilon)
    normed = centred * inverse
    return (normed * scales, normed, inverse)


def layer_backward(upstream, scales, normed, inverse):
    scaled = upstream * scales
    first_moment = jnp.mean(scaled, axis=-1, keepdims=True)
    second_moment = jnp.mean(scaled * normed, axis=-1, keepdims=True)
    return inverse * (scaled - first_moment - normed * second_moment)


LOADED = ("noisy", "single", "restype", "table", "ng", "pair", "pg", "wp", "chain", "keymask")
LOADED += ("wq", "wk", "wv", "cot", "wdown", "wo", "tg", "wgate", "wup")
INPUTS = tuple(n + "_h" for n in LOADED) + ("cw",)
OUTPUTS = ("gn_o", "ogs", "gp_o", "owg", "opw")
OUT_SHAPES = (
    ((128, 768), BF),
    ((2, 24, 128), F32),
    ((128, 32, 128), BF),
    ((3, 24, 128), BF),
    ((8, 128), F32),
)
V = pltpu.VMEM
SCRATCH = dict(
    wq=V((768, 768), BF),
    wk=V((768, 768), BF),
    wv=V((768, 768), BF),
    wo=V((768, 768), BF),
    wgate=V((768, 1536), BF),
    wup=V((768, 1536), BF),
    wdown=V((1536, 768), BF),
    noisy=V((128, 768), BF),
    single=V((128, 768), BF),
    restype=V((1, 128), jnp.int32),
    table=V((32, 768), BF),
    ng=V((768,), F32),
    pair=V((128, 32, 128), BF),
    pg=V((1, 128), F32),
    wp=V((8, 128), BF),
    chain=V((8, 128), jnp.int32),
    keymask=V((8, 128), jnp.int32),
    cot=V((128, 768), BF),
    tg=V((768,), F32),
    pairs=V((32 * 136, 128), F32),
    das=V((8, 96, 128), BF),
    dat=V((8, 96, 128), BF),
    g2=V((8, 4096), F32),
    gn=V((128, 768), BF),
    gp=V((128, 32, 128), BF),
    load=pltpu.SemaphoreType.DMA((19,)),
    store=pltpu.SemaphoreType.DMA((2,)),
    send=pltpu.SemaphoreType.DMA((180,)),
    recv=pltpu.SemaphoreType.DMA((180,)),
    xs=V((128, 768), BF),
    xf=V((8, 128, 768), BF),
    pr=V((32, 128, 128), BF),
    bj=V((256, 128), F32),
    bt=V((8, 32, 128), BF),
    f=V((32, 8, 32, 128), BF),
    ab=V((1024, 128), F32),
    bb=V((1024, 128), F32),
    cb=V((1024, 128), F32),
    q=V((1024, 128), BF),
    k=V((1024, 128), BF),
    v=V((1024, 128), BF),
    kt=V((128, 1024), BF),
    vt=V((128, 1024), BF),
    pt=V((8, 1024, 128), BF),
    att=V((8, 96, 128), BF),
    attl=V((8, 96, 128), BF),
    dh=V((128, 1536), F32),
    dres=V((128, 768), F32),
    drs=V((768, 128), BF),
    dr=V((8, 768, 128), BF),
    dq=V((8, 3, 96, 128), BF),
    odq=V((3, 8, 96, 128), BF),
    db=V((16, 2, 8, 32, 128), BF),
    dk=V((1024, 128), F32),
    dv=V((1024, 128), F32),
    go=V((768, 96), F32),
    zz=V((288, 1024), BF),
    wg=V((2, 16, 3, 24, 128), BF),
    wg1=V((16, 3, 24, 128), BF),
    ws=V((16, 3, 24, 128), BF),
    gt=V((3, 24, 128), BF),
    db1=V((16, 2, 4, 32, 128), BF),
    s1=V((16, 2, 4, 32, 128), BF),
    bu=V((2, 4, 32, 128), BF),
    bl=V((8, 32, 128), BF),
    odb=V((8, 32, 128), BF),
    gj=V((256, 128), F32),
    gs=V((2, 16, 2, 24, 128), BF),
    gs1=V((16, 2, 24, 128), BF),
    ss=V((16, 2, 24, 128), BF),
    p0=V((8, 128), F32),
    p1=V((8, 128), F32),
    p2=V((8, 128), F32),
    p3=V((8, 128), F32),
    r0=V((8, 128), F32),
    r1=V((3, 8, 128), F32),
    r2=V((3, 8, 128), F32),
    r3=V((8, 8, 128), F32),
)
for name, rest in (("bw", (3, 24, 128)), ("bd", (2, 4, 32, 128)), ("bg", (2, 24, 128))):
    for at, ref in enumerate(scatter_scratch(rest)):
        SCRATCH[name + str(at)] = ref


class Refs:
    pass


def block_kernel(*refs):
    r = Refs()
    for name, ref in zip(INPUTS + OUTPUTS + tuple(SCRATCH), refs):
        setattr(r, name, ref)
    me = Place()
    w = Wire(r.send, r.recv)
    h = me.tok
    scale = 96**-0.5
    toks = [me.tok_at(d) for d in range(1, 8)]
    turn = me.tok * 4 + lax.rem(me.copy, 4)
    turn_tok = me.copy // 4
    other = turn_tok != me.tok
    partner = {
        "copy_0": turn // 8,
        "copy_1": lax.rem(turn // 2, 4),
        "copy_2": lax.rem(turn, 2),
        "tok_0": turn_tok // 4,
        "tok_1": lax.rem(turn_tok, 4),
    }

    barrier = pltpu.get_barrier_semaphore()
    peers = [d for _, d in toks] + [me.other_core()]
    peers += [me.around_z(k) for k in (1, 2, 3)] + [me.around_y(k) for k in (1, 2, 3)]
    for d in peers:
        pl.semaphore_signal(barrier, inc=1, device_id=d, device_id_type=MESH)

    @pl.when(other)
    def _():
        pl.semaphore_signal(barrier, inc=1, device_id=partner, device_id_type=MESH)

    loads = {}
    for n, name in enumerate(LOADED):
        c = pltpu.make_async_copy(getattr(r, name + "_h"), getattr(r, name), r.load.at[n])
        c.start()
        loads[name] = c

    def ready(*names):
        for name in names:
            loads[name].wait()

    ready("noisy", "single", "restype", "table", "ng")
    gain = r.ng[...].reshape(1, 768)
    noisy_f = r.noisy[...].astype(F32)
    classes = lax.broadcasted_iota(jnp.int32, (32, 128), 0) == r.restype[...]
    classes = jnp.where(classes, 1.0, 0.0).astype(BF)
    condition = r.single[...].astype(F32) + dot(classes, r.table[...], 0, 0)
    x = (layer_forward(noisy_f, gain)[0] + condition).astype(BF)
    r.xs[...] = x
    r.xf[me.tok] = x

    ready("pair", "pg", "wp")

    @pl.loop(0, 16)
    def _(n):
        for m in range(8):
            i = n * 8 + m
            r.pairs[pl.ds(i, 32, stride=136)] = r.pair[i].astype(F32)

    def column(j):
        return pl.ds(pl.multiple_of(j * 136, 8), 128)

    @pl.loop(0, 8)
    def _(n):
        for m in range(4):
            j = n * 4 + m
            p = layer_forward(r.pairs[column(j)], r.pg[...])[0].astype(BF)
            r.pr[j] = p
            r.bj[pl.ds(pl.multiple_of(j * 8, 8), 8)] = dot(r.wp[...], p, 1, 1)

    for n in range(8):
        r.bt[n] = r.bj[pl.ds(n, 32, stride=8)].astype(BF)
    pl.semaphore_wait(barrier, len(peers) + jnp.where(other, 1, 0))
    bs = bias_chain(w, me, r.bt, r.f, toks)
    step(bs)
    xs = gather_chain(w, me, r.xs, r.xf, 128)
    step(xs)
    ready("chain", "keymask")
    for t in range(8):
        code = jnp.where(r.keymask[t : t + 1] > 0, r.chain[t : t + 1], r.chain[t : t + 1] + 8)
        code = jnp.broadcast_to(code.astype(F32), (128, 128)).T
        rows = pl.ds(t * 128, 128)
        r.cb[rows] = code
        same = jnp.zeros((128, 128), F32)
        for c in range(6):
            same = jnp.where(code == c, r.cw[c, h], same)
        r.ab[rows] = same
        r.bb[rows] = jnp.where(code >= 8, -1e30, 0.0)
    step(bs)
    ready("wq", "wk", "wv")
    row = lax.broadcasted_iota(jnp.int32, (768, 128), 0)
    col = lax.broadcasted_iota(jnp.int32, (768, 128), 1)
    pick = jnp.where((row == col + h * 96) & (col < 96), 1.0, 0.0).astype(BF)
    heads = [dot(m[...], pick).astype(BF) for m in (r.wq, r.wk, r.wv)]

    def project(t):
        rows = pl.ds(pl.multiple_of(t * 128, 128), 128)
        for m, o in zip(heads, (r.q, r.k, r.v)):
            o[rows] = dot(r.xf[t], m).astype(BF)

    step(bs)
    step(xs)
    ready("cot", "wdown")
    r.dh[...] = dot(r.cot[...], r.wdown[...], 1, 1)
    step(bs)
    step(xs)
    step(bs, 2)
    step(xs)
    for t in range(4):
        project(me.zh * 4 + t)
    step(bs, 2)
    step(xs)
    step(bs, 3)
    step(xs)
    for t in range(4):
        project((1 - me.zh) * 4 + t)
    r.vt[...] = r.v[...].T
    r.kt[...] = r.k[...].T
    turns(bs, xs)

    ak = w.take(7)

    def att_copy(s, t):
        device = {"tok_0": t // 4, "tok_1": lax.rem(t, 4)}
        return w.copy(r.att.at[t], r.attl.at[me.tok], device, ak + s)

    @pl.loop(0, 8)
    def _(s):
        t = lax.rem(me.tok + 1 + s, 8)

        @pl.when(s > 0)
        def _():
            att_copy(s - 1, lax.rem(me.tok + s, 8)).start()

        rows = pl.ds(pl.multiple_of(t * 128, 128), 128)
        a = dot(r.k[...], r.q[rows], 1, 1)
        bias = r.f[:, t].reshape(1024, 128).astype(F32)
        own = r.chain[pl.ds(t, 1)].astype(F32)
        a = a * scale + (bias + jnp.where(r.cb[...] == own, r.ab[...], r.bb[...]))
        e = jnp.exp(a - jnp.max(a, axis=0, keepdims=True))
        p = (e * (1.0 / jnp.sum(e, axis=0, keepdims=True))).astype(BF)
        r.pt[t] = p
        r.att[t] = dot(r.vt[...], p)[:96].astype(BF)

    r.attl[me.tok] = r.att[me.tok]
    for s in range(7):
        att_copy(s, toks[s][0]).wait()

    ready("wo", "tg", "wgate", "wup")
    trans_gain = r.tg[...].reshape(1, 768)
    residual = noisy_f + dot(r.attl[...].reshape(768, 128), r.wo[...], 0, 0)
    scaled, trans_hat, trans_inverse = layer_forward(residual, trans_gain)
    trans_in = scaled.astype(BF)
    d_trans = jnp.zeros((128, 768), F32)
    for n in range(3):
        cols = pl.ds(n * 512, 512)
        gate = dot(trans_in, r.wgate[:, cols])
        up = dot(trans_in, r.wup[:, cols])
        d_hidden = r.dh[:, cols]
        sig = 1.0 / (1.0 + jnp.exp(-gate))
        d_gate = (d_hidden * up * sig * (1.0 + gate * (1.0 - sig))).astype(BF)
        d_up = (d_hidden * gate * sig).astype(BF)
        d_trans = d_trans + dot(d_gate, r.wgate[:, cols], 1, 1) + dot(d_up, r.wup[:, cols], 1, 1)
    d_res = r.cot[...].astype(F32) + layer_backward(d_trans, trans_gain, trans_hat, trans_inverse)
    r.dres[...] = d_res
    d_att = dot(r.wo[...], d_res.astype(BF), 1, 1)
    r.das[...] = d_att.astype(BF).reshape(8, 96, 128)
    d_res_t = d_res.T.astype(BF)
    r.drs[...] = d_res_t
    r.dr[me.tok] = d_res_t
    fan = [w.go(r.das.at[t], r.dat.at[me.tok], d) for t, d in toks]
    r.dat[me.tok] = r.das[me.tok]
    ds = gather_chain(w, me, r.drs, r.dr, 768)
    step(ds)
    r.dk[...] = jnp.zeros_like(r.dk)
    r.dv[...] = jnp.zeros_like(r.dv)
    r.go[...] = jnp.zeros_like(r.go)
    r.wg[...] = jnp.zeros_like(r.wg)
    r.gs[...] = jnp.zeros_like(r.gs)
    for c in fan:
        c.wait_recv()

    def back(t):
        rows = pl.ds(pl.multiple_of(t * 128, 128), 128)
        d_att = jnp.concatenate([r.dat[t], jnp.zeros((32, 128), BF)], axis=0)
        p = r.pt[t]
        dp = dot(r.v[...], d_att)
        pf = p.astype(F32)
        dsb = (pf * (dp - jnp.sum(pf * dp, axis=0, keepdims=True))).astype(BF)
        r.db[:, :, t] = dsb.reshape(16, 2, 32, 128)
        dqt = (dot(r.kt[...], dsb)[:96] * scale).astype(BF)
        r.dq[t, 0] = dqt
        r.zz[0:96, rows] = dqt
        r.dv[...] += dot(p, d_att.astype(F32).T.astype(BF))
        r.dk[...] += dot(dsb, r.q[rows])


    @pl.loop(0, 4)
    def _(n):
        back(4 * (1 - me.core) + n)

    mine = pl.ds(4 * me.core, 4)
    theirs = pl.ds(4 * (1 - me.core), 4)

    def bias_sum():
        c = w.go(r.db.at[:, :, theirs], r.db1, me.other_core())
        yield 1
        c.wait_recv()

        @pl.loop(0, 16)
        def _(n):
            r.s1[n] = (r.db[n, :, mine].astype(F32) + r.db1[n].astype(F32)).astype(BF)

        def done(total):
            r.bu[...] = total.astype(BF)

        yield from scatter_chain(w, me, r.s1, [getattr(r, "bd" + str(n)) for n in range(5)], done)
        c = w.go(r.bu.at[1 - me.core], r.bl.at[mine], me.other_core())
        r.bl[mine] = r.bu[me.core]
        yield 1
        c.wait_recv()
        fan = [w.go(r.bl.at[t], r.odb.at[me.tok], d) for t, d in toks]
        r.odb[me.tok] = r.bl[me.tok]
        yield 1
        for c in fan:
            c.wait_recv()

    bsum = bias_sum()
    step(bsum)
    step(ds)

    @pl.loop(0, 4)
    def _(n):
        back(4 * me.core + n)

    step(bsum)
    step(ds)
    dkt = (r.dk[...] * scale).T[:96].astype(BF)
    dvt = r.dv[...].T[:96].astype(BF)
    for t in range(8):
        r.dq[t, 1] = dkt[:, t * 128 : (t + 1) * 128]
        r.dq[t, 2] = dvt[:, t * 128 : (t + 1) * 128]
    r.zz[96:192] = dkt
    r.zz[192:288] = dvt
    moves = [w.go(r.dq.at[t], r.odq.at[:, me.tok], d) for t, d in toks]
    r.odq[:, me.tok] = r.dq[me.tok]

    xf = r.xf[...].reshape(1024, 768)
    for s in range(3):
        g = dot(r.zz[s * 96 : (s + 1) * 96], xf)
        for te in range(8):
            part = g[:, te * 96 : (te + 1) * 96].astype(BF)
            for j in range(4):
                r.wg[j % 2, 2 * te + j // 2, s, :, 0:96] = part[j * 24 : (j + 1) * 24]
    tk = w.take(1)

    def turned():
        return w.copy(r.gt, r.owg, partner, tk)

    def weight_sum():
        c = w.go(r.wg.at[1 - me.core], r.wg1, me.other_core())
        yield 1
        c.wait_recv()
        r.ws[...] = (r.wg[me.core].astype(F32) + r.wg1[...].astype(F32)).astype(BF)

        def done(total):
            r.gt[...] = total.astype(BF)

        yield from scatter_chain(w, me, r.ws, [getattr(r, "bw" + str(n)) for n in range(5)], done)
        @pl.when(other)
        def _():
            turned().start()

        @pl.when(jnp.logical_not(other))
        def _():
            r.owg[...] = r.gt[...]

    wsum = weight_sum()
    step(wsum)
    step(bsum)
    step(ds)
    step(wsum)
    step(ds)
    step(bsum)
    turns(ds)

    @pl.loop(0, 8)
    def _(t):
        r.go[...] += dot(r.dr[t], r.att[t].astype(F32).T.astype(BF))

    for n in range(32):
        r.gs[n % 2, n // 2, 1, :, 0:96] = r.go[n * 24 : (n + 1) * 24].astype(BF)
    step(wsum)
    step(bsum)
    for c in moves:
        c.wait_recv()
    odq = r.odq[...].reshape(3, 768, 128)
    d_in_t = dot(r.wq[...], odq[0]) + dot(r.wk[...], odq[1]) + dot(r.wv[...], odq[2])
    for n in range(32):
        r.gs[n % 2, n // 2, 0] = d_in_t[n * 24 : (n + 1) * 24].astype(BF)

    def single_sum():
        c = w.go(r.gs.at[1 - me.core], r.gs1, me.other_core())
        yield 1
        c.wait_recv()
        r.ss[...] = (r.gs[me.core].astype(F32) + r.gs1[...].astype(F32)).astype(BF)

        def done(total):
            r.ogs[...] = total

        yield from scatter_chain(w, me, r.ss, [getattr(r, "bg" + str(n)) for n in range(5)], done)

    gsum = single_sum()
    step(gsum)
    step(bsum)
    step(wsum)
    step(gsum)
    scaled, noisy_hat, noisy_inverse = layer_forward(r.noisy[...].astype(F32), gain)
    r.gn[...] = (
        r.dres[...] + layer_backward(d_in_t.T, gain, noisy_hat, noisy_inverse)
    ).astype(BF)
    step(wsum)
    step(gsum)
    turns(bsum)

    for n in range(8):
        r.gj[pl.ds(n, 32, stride=8)] = r.odb[n].astype(F32)
    for n in range(32):
        r.g2[:, n * 128 : (n + 1) * 128] = r.gj[n * 8 : (n + 1) * 8]
    r.p3[...] = dot(r.g2[...].astype(BF), r.pr[...].reshape(4096, 128))

    def in_order(own, got, at):
        terms = []
        for k in range(4):
            d = lax.rem(at + 4 - k, 4)
            term = jnp.where(d == 0, own[...], jnp.zeros_like(own[...]))
            for j in (1, 2, 3):
                term = jnp.where(d == j, got[j - 1], term)
            terms.append(term)
        return (terms[0] + terms[1]) + (terms[2] + terms[3])

    def pair_weight_sum():
        c = w.go(r.p3, r.r0, me.other_core())
        yield 1
        c.wait_recv()
        r.p0[...] = r.p3[...] + r.r0[...]
        zs = [w.go(r.p0, r.r1.at[k - 1], me.around_z(k)) for k in (1, 2, 3)]
        yield 1
        for c in zs:
            c.wait_recv()
        r.p1[...] = in_order(r.p0, r.r1, me.z)
        ys = [w.go(r.p1, r.r2.at[k - 1], me.around_y(k)) for k in (1, 2, 3)]
        yield 1
        for c in ys:
            c.wait_recv()
        r.p2[...] = in_order(r.p1, r.r2, me.y)
        ts = [w.go(r.p2, r.r3.at[me.tok], d) for _, d in toks]
        r.r3[me.tok] = r.p2[...]
        yield 1
        for c in ts:
            c.wait_recv()
        total = r.r3[0]
        for k in range(1, 8):
            total = total + r.r3[k]
        r.opw[...] = total

    psum = pair_weight_sum()
    for n in range(4):
        step(psum)
        if n in (1, 2):
            step(gsum)

        @pl.loop(n * 2, n * 2 + 2)
        def _(b):
            for m in range(4):
                j = b * 4 + m
                g = r.gj[pl.ds(pl.multiple_of(j * 8, 8), 8)].astype(BF)
                up = dot(g, r.wp[...], 0, 0)
                hat, inverse = layer_forward(r.pairs[column(j)], r.pg[...])[1:]
                r.pairs[column(j)] = layer_backward(up, r.pg[...], hat, inverse)

    @pl.loop(0, 16)
    def _(n):
        for m in range(8):
            i = n * 8 + m
            r.gp[i] = r.pairs[pl.ds(i, 32, stride=136)].astype(BF)

    w.close()
    stores = [
        pltpu.make_async_copy(r.gn, r.gn_o, r.store.at[0]),
        pltpu.make_async_copy(r.gp, r.gp_o, r.store.at[1]),
    ]
    for c in stores:
        c.start()
    turns(psum, wsum, gsum)

    @pl.when(other)
    def _():
        turned().wait()

    for c in stores:
        c.wait()
    w.close()


def whole_block(*args):
    spaces = [pl.BlockSpec(memory_space=pl.ANY)] * len(LOADED)
    spaces += [pl.BlockSpec(memory_space=pltpu.SMEM)]
    return pl.pallas_call(
        block_kernel,
        out_shape=[jax.ShapeDtypeStruct(s, d) for s, d in OUT_SHAPES],
        in_specs=spaces,
        out_specs=[spaces[0], VM, spaces[0], VM, VM],
        scratch_shapes=list(SCRATCH.values()),
        compiler_params=pltpu.CompilerParams(
            collective_id=0, has_side_effects=True, vmem_limit_bytes=62 << 20
        ),
    )(*args)


def results_kernel(gn, ogs, gp, owg, opw, *rest):
    outs, (vgn, vgp, vogs, vowg, vopw, sem) = rest[:8], rest[8:]
    ogn, osingle, ogp, oq, ok, ov, oo, opair = outs
    ins = [pltpu.make_async_copy(gp.at[pl.ds(n * 32, 32)], vgp.at[n], sem.at[n]) for n in range(4)]
    ins.append(pltpu.make_async_copy(gn, vgn, sem.at[4]))
    small = [
        pltpu.make_async_copy(a, b, sem.at[5 + n])
        for n, (a, b) in enumerate(((ogs, vogs), (owg, vowg), (opw, vopw)))
    ]
    for c in ins + small:
        c.start()
    back = [
        pltpu.make_async_copy(vgp.at[n], ogp.at[pl.ds(n * 32, 32)], sem.at[8 + n])
        for n in range(4)
    ]
    back.append(pltpu.make_async_copy(vgn, ogn, sem.at[12]))
    for a, b in zip(ins, back):
        a.wait()
        b.start()
    for c in small:
        c.wait()
    osingle[...] = vogs[0]
    for n, o in enumerate((oq, ok, ov)):
        o[...] = vowg[n, :, 0:96].astype(F32)
    oo[...] = vogs[1, :, 0:96]
    opair[...] = vopw[...]
    for c in back:
        c.wait()


def results(*args):
    grad = jax.ShapeDtypeStruct((24, 96), F32)
    anywhere = pl.BlockSpec(memory_space=pl.ANY)
    return pl.pallas_call(
        results_kernel,
        out_shape=[
            jax.ShapeDtypeStruct((128, 768), BF),
            jax.ShapeDtypeStruct((24, 128), F32),
            jax.ShapeDtypeStruct((128, 32, 128), BF),
            grad,
            grad,
            grad,
            grad,
            jax.ShapeDtypeStruct((8, 128), F32),
        ],
        in_specs=[anywhere] * 5,
        out_specs=[anywhere, VM, anywhere, VM, VM, VM, VM, VM],
        scratch_shapes=[
            V((128, 768), BF),
            V((4, 32, 32, 128), BF),
            V((2, 24, 128), F32),
            V((3, 24, 128), BF),
            V((8, 128), F32),
            pltpu.SemaphoreType.DMA((13,)),
        ],
        compiler_params=pltpu.CompilerParams(vmem_limit_bytes=60 << 20),
    )(*args)


def per_device(
    noisy,
    single,
    pair,
    restype,
    chain,
    keymask,
    restype_table,
    norm_gain,
    pair_gain,
    trans_gain,
    w_query,
    w_key,
    w_value,
    w_out,
    w_pair,
    chain_weight,
    w_hidden_gate,
    w_hidden_up,
    w_down,
    cotangent,
):
    parts = whole_block(
        noisy[0],
        single,
        restype.reshape(1, 128),
        restype_table,
        norm_gain,
        pair,
        pair_gain.reshape(1, 128),
        w_pair.T,
        chain.reshape(8, 128),
        keymask.reshape(8, 128),
        w_query,
        w_key,
        w_value,
        cotangent[0],
        w_down,
        w_out,
        trans_gain,
        w_hidden_gate,
        w_hidden_up,
        chain_weight,
    )
    gn, gsingle, gp, gq, gk, gv, gout, gpw = results(*parts)
    return gn[None], gsingle.T, gp, gq.T, gk.T, gv.T, gout.T, gpw.T


def solution(mesh):
    torus = Mesh(
        mesh.devices.reshape(4, 4, 2, 2, 4), ("copy_0", "copy_1", "copy_2", "tok_0", "tok_1")
    )
    return jax.shard_map(
        per_device,
        mesh=torus,
        in_specs=(
            P(COPY, TOK, None),
            P(TOK, None),
            P(TOK, COPY, None),
            P(TOK),
            P(),
            P(),
            P(),
            P(),
            P(),
            P(),
            P(),
            P(),
            P(),
            P(),
            P(),
            P(),
            P(),
            P(),
            P(),
            P(COPY, TOK, None),
        ),
        out_specs=(
            P(COPY, TOK, None),
            P(TOK, COPY),
            P(TOK, COPY, None),
            P(TOK, COPY),
            P(TOK, COPY),
            P(TOK, COPY),
            P(TOK, COPY),
            P(),
        ),
        check_vma=False,
    )
```
